256 devices in a mesh: row: 8 (over z), col: 32 (over x, y, core).
Axes of the slice: x: 4, y: 4, z: 8, core: 2. Of those that a mesh axis runs over, the one named last changes fastest.
Arguments:
- tile_values: bfloat16 [8, 32, 128, 128, 128], P('row', 'col'), may hold values from -0.1875 to 0.1875
- tile_rows: int32 [8, 32, 128], P('row', 'col'), may hold values from 0 to 15, as said below
- tile_cols: int32 [8, 32, 128], P('row', 'col'), may hold values from 0 to 15, as said below
- tile_count: int32 [8, 32], P('row', 'col'), may hold values from 42 to 128, as said below
- sinogram: float32 [16384, 128], P('row'), may hold values from -6 to 6
Outputs:
- solution: float32 [65536, 128], P('col')
- residual_estimate: float32 [128], replicated
The draws below stay inside these ranges and needn't reach their ends.
Inputs may be any that keep to these rules, and one draw needn't show every extreme that they name: On each device the 128 slots name distinct tile positions (tile_rows, tile_cols) of its grid of 16 x 16 tiles. `tile_cols`: see tile_rows. `tile_count`: some device holds 128 tiles in every draw.
All inputs are finite; a program needn't handle non-finite values.
Results may differ from the reference program's by a relative error of at most 0.0019.
Values may be sent and summed in bfloat16 or wider, within the bound.
A program may use at most 128 MiB of HBM per device.

```python
import jax
import jax.numpy as jnp
from jax import lax

TILE = 128
TR = 16
TC = 16
CAP = 128
Z = 128
ITERS = 3
M = 16384
N_ROW = 8
N_COL = 32


def occupancy(key):
    base = jax.random.fold_in(key, 7)
    device_keys = jax.random.split(base, N_ROW * N_COL)
    orders = jax.vmap(lambda single: jax.random.permutation(single, TR * TC))(device_keys)
    return orders[:, :CAP].reshape(N_ROW, N_COL, CAP).astype(jnp.int32)


def draw_tile_rows(key, part):
    return (occupancy(key) // TC).astype(jnp.int32)


def draw_tile_cols(key, part):
    return (occupancy(key) % TC).astype(jnp.int32)


def draw_tile_count(key, part):
    counts = jax.random.randint(jax.random.fold_in(key, 11), (N_ROW * N_COL,), CAP // 3, CAP + 1)
    fullest = jax.random.randint(jax.random.fold_in(key, 13), (), 0, N_ROW * N_COL)
    flat = jnp.where(jnp.arange(N_ROW * N_COL) == fullest, CAP, counts)
    return flat.reshape(N_ROW, N_COL).astype(jnp.int32)


def steps_of(stream_key, shape, pieces, least, top_value):
    factor_of = 1.0
    for position, parts in pieces:
        steps = jax.random.uniform(jax.random.fold_in(jax.random.fold_in(stream_key, 6), position), (parts,), jnp.float32, least / len(pieces), top_value / len(pieces))
        factor_of = factor_of * jnp.repeat(jnp.exp(steps), shape[position] // parts).reshape((-1,) + (1,) * (len(shape) - 1 - position))
    return factor_of


def scatter_about(stream_key, extent, scale, limit, cuts=(), kind=jnp.bfloat16):
    entries = scale * jax.random.normal(stream_key, extent, jnp.float32)
    if cuts:
        entries = entries * steps_of(stream_key, extent, cuts, -0.22, 0.18)
    return jnp.clip(entries, -limit, limit).astype(kind)


def setup_inputs(seed: int = 0) -> dict:
    arg_keys = jax.random.split(jax.random.key(seed), 6)
    return {
        "tile_values": scatter_about(arg_keys[0], (N_ROW, N_COL, CAP, TILE, TILE), (TILE * CAP // TR) ** -0.5, 0.1875, ((0, 8), (1, 32))),
        "tile_rows": draw_tile_rows(jax.random.fold_in(arg_keys[5], 71), 0),
        "tile_cols": draw_tile_cols(jax.random.fold_in(arg_keys[5], 71), 0),
        "tile_count": draw_tile_count(jax.random.fold_in(arg_keys[5], 71), 0),
        "sinogram": scatter_about(arg_keys[4], (M, Z), 1.0, 6.0, ((0, 8),), jnp.float32),
    }


EPSILON = 1e-06

def column_norm(vec):
    return jnp.sqrt(lax.optimization_barrier(jnp.sum(vec * vec, axis=0)) + EPSILON)

def project(tile_values, tile_rows, tile_cols, tile_count, source, forward):
    operand = source.astype(jnp.bfloat16).astype(jnp.float32)
    slot_ids = jnp.arange(CAP, dtype=jnp.int32)
    if forward:
        out_rows = TR * TILE * N_ROW
        out_blocks = TR
        in_len = TC * TILE
        pattern = 'tij,tjz->tiz'
    else:
        out_rows = TC * TILE * N_COL
        out_blocks = TC
        in_len = TR * TILE
        pattern = 'tji,tjz->tiz'

    def one_device(carry, device_idx):
        row_idx = device_idx // N_COL
        col_idx = device_idx % N_COL
        values = tile_values[row_idx, col_idx].astype(jnp.float32)
        if forward:
            take_index = tile_cols[row_idx, col_idx]
            put_index = tile_rows[row_idx, col_idx]
            in_first = (col_idx * in_len).astype(jnp.int32)
            out_first = (row_idx * (out_blocks * TILE)).astype(jnp.int32)
        else:
            take_index = tile_rows[row_idx, col_idx]
            put_index = tile_cols[row_idx, col_idx]
            in_first = (row_idx * in_len).astype(jnp.int32)
            out_first = (col_idx * (out_blocks * TILE)).astype(jnp.int32)
        blocks = lax.dynamic_slice_in_dim(operand, in_first, in_len, 0).reshape(in_len // TILE, TILE, Z)
        products = jnp.einsum(pattern, values, blocks[take_index], precision=lax.Precision.HIGHEST)
        live_mask = (slot_ids < tile_count[row_idx, col_idx]).astype(jnp.float32)
        targets = jnp.arange(out_blocks, dtype=jnp.int32)
        onehot = (put_index[None, :] == targets[:, None]).astype(jnp.float32) * live_mask[None, :]
        part_sum = jnp.einsum('rt,tiz->riz', onehot, products, precision=lax.Precision.HIGHEST)
        part_sum = part_sum.reshape(out_blocks * TILE, Z)
        current = lax.dynamic_slice_in_dim(carry, out_first, out_blocks * TILE, 0)
        return (lax.dynamic_update_slice_in_dim(carry, current + part_sum, out_first, 0), None)
    start = jnp.zeros((out_rows, Z), jnp.float32)
    result, unused = lax.scan(one_device, start, jnp.arange(N_ROW * N_COL, dtype=jnp.int32))
    return result

def rotation(rho_bar, beta_norm, phi_bar):
    rho_value = jnp.sqrt(rho_bar * rho_bar + beta_norm * beta_norm)
    cosine = rho_bar / rho_value
    sine_value = beta_norm / rho_value
    return (rho_value, cosine, sine_value, cosine * phi_bar, sine_value * phi_bar)

def reference(tile_values, tile_rows, tile_cols, tile_count, sinogram):
    beta_norm = column_norm(sinogram)
    ray_vec = sinogram / beta_norm
    voxel_raw = project(tile_values, tile_rows, tile_cols, tile_count, sinogram, False) / beta_norm
    alpha_norm = column_norm(voxel_raw)
    voxel_vec = voxel_raw / alpha_norm
    search_dir = voxel_vec
    solution = jnp.zeros_like(voxel_vec)
    phi_bar = beta_norm
    rho_bar = alpha_norm
    for step_idx in range(ITERS):
        ray_raw = project(tile_values, tile_rows, tile_cols, tile_count, voxel_raw, True) / alpha_norm - alpha_norm * ray_vec
        beta_norm = column_norm(ray_raw)
        ray_vec = ray_raw / beta_norm
        rho_value, cosine, sine_value, phi_value, phi_bar = rotation(rho_bar, beta_norm, phi_bar)
        solution = solution + phi_value / rho_value * search_dir
        if step_idx + 1 < ITERS:
            voxel_raw = project(tile_values, tile_rows, tile_cols, tile_count, ray_raw, False) / beta_norm - beta_norm * voxel_vec
            alpha_norm = column_norm(voxel_raw)
            voxel_vec = voxel_raw / alpha_norm
            theta_value = sine_value * alpha_norm
            rho_bar = -cosine * alpha_norm
            search_dir = voxel_vec - theta_value / rho_value * search_dir
    return (solution, phi_bar)
```

```python
import functools

import jax
import jax.numpy as jnp
from jax import lax
from jax.experimental import pallas as pl
from jax.experimental.pallas import tpu as pltpu
from jax.sharding import Mesh
from jax.sharding import PartitionSpec as P

ITERS = 3
NZ = 8
NX = 4
NY = 4
NQ = NX * NY
TILE = 128
Z = 128
BLK = 2048
VB = BLK // NZ
HALF = BLK // 2
RB = HALF // NQ
EPSILON = 1e-06
MESH = pl.DeviceIdType.MESH
F32 = jnp.float32
BF16 = jnp.bfloat16


def squares8(x):
    return jnp.sum((x * x).reshape(-1, 8, Z), axis=0)


def kernel(
    inv,
    values,
    sino,
    out,
    residual,
    dense,
    rays_t,
    quant,
    quant_meta,
    back,
    back_meta,
    own_back,
    high,
    low,
    high_ss,
    part_own,
    part_out,
    part_in,
    part_ss,
    fwd_out,
    fwd_in,
    fwd_ss,
    rays,
    rays_ss,
    half_ss,
    last_ss,
    z_send,
    z_recv,
    zm_send,
    zm_recv,
    h_send,
    h_recv,
    hs_send,
    hs_recv,
    l_send,
    l_recv,
    c_send,
    c_recv,
    q_send,
    q_recv,
    qs_send,
    qs_recv,
    g_send,
    g_recv,
    gs_send,
    gs_recv,
    k_send,
    k_recv,
    e_send,
    e_recv,
):
    z = lax.axis_index("row")
    cx = lax.axis_index("cx")
    cy = lax.axis_index("cy")
    core = lax.axis_index("cc")
    chip = cx * NY + cy

    def z_peer(step):
        return lax.rem(z + step, NZ)

    def z_id(step):
        return {"row": lax.rem(z + step, NZ)}

    def chip_at(step):
        return lax.rem(cx + step // NY, NX), lax.rem(cy + lax.rem(step, NY), NY)

    def chip_id(step):
        px, py = chip_at(step)
        return {"cx": px, "cy": py}

    def chip_peer(step):
        px, py = chip_at(step)
        return px * NY + py

    other = {"cc": 1 - core}

    barrier = pltpu.get_barrier_semaphore()

    def greet_z(step, carry):
        pl.semaphore_signal(barrier, inc=1, device_id=z_id(step), device_id_type=MESH)
        return carry

    def greet_chip(step, carry):
        pl.semaphore_signal(barrier, inc=1, device_id=chip_id(step), device_id_type=MESH)
        return carry

    lax.fori_loop(1, NZ, greet_z, 0)
    lax.fori_loop(1, NQ, greet_chip, 0)
    pl.semaphore_signal(barrier, inc=1, device_id=other, device_id_type=MESH)

    def remote(src, dst, send, recv, device):
        return pltpu.make_async_remote_copy(
            src_ref=src, dst_ref=dst, send_sem=send, recv_sem=recv, device_id=device, device_id_type=MESH
        )

    def fill(i, carry):
        at = pl.ds(pl.multiple_of(i * TILE, TILE), TILE)
        for j in range(BLK // TILE):
            slot = inv[i * (BLK // TILE) + j]
            tile = values[jnp.maximum(slot, 0)]
            tile = jnp.where(slot >= 0, tile, jnp.zeros_like(tile))
            dense[j // 2, at, (j % 2) * TILE : (j % 2 + 1) * TILE] = tile
        return carry

    lax.fori_loop(0, BLK // TILE, fill, 0)

    def read_sino(i, total):
        at = pl.ds(pl.multiple_of(i * 256, 256), 256)
        block = sino[at, :]
        rays_t[:, at] = block.T.astype(BF16)
        return total + squares8(block)

    row_ss = lax.fori_loop(0, BLK // 256, read_sino, jnp.zeros((8, Z), F32))

    def backward(turn, row_ss):
        def product(p):
            block = jnp.dot(rays_t[...], dense[p], preferred_element_type=F32)
            return block.T

        def z_copies(step, to):
            p = z_peer(step)
            src = z_peer(NZ - step)
            data = remote(quant.at[turn, p], back.at[turn, z if to else src], z_send.at[turn, step], z_recv.at[turn, step], z_id(step))
            meta = remote(
                quant_meta.at[turn, p], back_meta.at[turn, z if to else src], zm_send.at[turn, step], zm_recv.at[turn, step], z_id(step)
            )
            return data, meta

        def give(i, carry):
            step = jnp.where(lax.rem(i, 2) == 0, NZ // 2 + i // 2, NZ // 2 - (i + 1) // 2)
            p = z_peer(step)
            block = product(p)
            top = jnp.maximum(jnp.max(jnp.abs(block), axis=0, keepdims=True), 1e-30)
            quant[turn, p] = jnp.round(block * (32767.0 / top)).astype(jnp.int32).astype(jnp.int16)
            quant_meta[turn, p, 0:8] = jnp.broadcast_to(top * (1.0 / 32767.0), (8, Z))
            quant_meta[turn, p, 8:16] = row_ss
            data, meta = z_copies(step, True)
            data.start()
            meta.start()
            return carry

        lax.fori_loop(0, NZ - 1, give, 0)
        own_back[...] = product(z)
        back_meta[turn, z, 8:16] = row_ss

        def take(step, carry):
            data, meta = z_copies(step, False)
            data.wait_recv()
            meta.wait_recv()
            src = z_peer(NZ - step)
            part = back[turn, src].astype(jnp.int32).astype(F32)
            own_back[...] += part * back_meta[turn, src, 0:1]
            return carry

        lax.fori_loop(1, NZ, take, 0)
        total = back_meta[turn, 0, 8:16]
        for i in range(1, NZ):
            total = total + back_meta[turn, i, 8:16]
        beta = jnp.sqrt(jnp.sum(total, axis=0, keepdims=True) + EPSILON)
        return beta

    def forward(turn, voxel):
        top = voxel.astype(BF16)
        high[turn, z] = top
        low[turn, z] = (voxel - top.astype(F32)).astype(BF16)
        high_ss[turn, z] = squares8(voxel)

        def high_copies(step, slot):
            data = remote(high.at[turn, z], high.at[turn, slot], h_send.at[turn, step], h_recv.at[turn, step], z_id(step))
            norm = remote(high_ss.at[turn, z], high_ss.at[turn, slot], hs_send.at[turn, step], hs_recv.at[turn, step], z_id(step))
            return data, norm

        def give(i, carry):
            step = jnp.where(lax.rem(i, 2) == 0, NZ // 2 + i // 2, NZ // 2 - (i + 1) // 2)
            data, norm = high_copies(step, z)
            data.start()
            norm.start()
            return carry

        lax.fori_loop(0, NZ - 1, give, 0)

        def take(step, carry):
            data, norm = high_copies(step, z_peer(NZ - step))
            data.wait_recv()
            norm.wait_recv()
            return carry

        lax.fori_loop(1, NZ, take, 0)

        def give_low(step, carry):
            remote(low.at[turn, z], low.at[turn, z], l_send.at[turn, step], l_recv.at[turn, step], z_id(step)).start()
            return carry

        lax.fori_loop(1, NZ, give_low, 0)

        total = high_ss[turn, 0]
        for i in range(1, NZ):
            total = total + high_ss[turn, i]
        part_ss[turn, 0] = total

        def product(first, i):
            at = pl.ds(pl.multiple_of(first + i * 256, 256), 256)
            block = jnp.dot(dense[0, at, :], high[turn, 0], preferred_element_type=F32)
            for p in range(1, NZ):
                block = block + jnp.dot(dense[p, at, :], high[turn, p], preferred_element_type=F32)
            return block.reshape(256 // RB, RB, Z)

        def core_copy(i):
            at = pl.ds(i * (256 // RB), 256 // RB)
            return remote(part_out.at[turn, at], part_in.at[turn, at], c_send.at[turn, i], c_recv.at[turn, i], other)

        core_norm = remote(part_ss.at[turn, 0], part_ss.at[turn, 1], k_send.at[turn], k_recv.at[turn], other)
        core_norm.start()

        def theirs(i, carry):
            part_out[turn, pl.ds(i * (256 // RB), 256 // RB)] = product((1 - core) * HALF, i)
            core_copy(i).start()
            return carry

        lax.fori_loop(0, HALF // 256, theirs, 0)

        def ours(i, carry):
            part_own[pl.ds(i * (256 // RB), 256 // RB)] = product(core * HALF, i)
            return carry

        lax.fori_loop(0, HALF // 256, ours, 0)
        core_norm.wait_recv()
        chip_ss = part_ss[turn, 0] + part_ss[turn, 1]
        fwd_ss[turn, chip] = chip_ss
        fwd_ss[turn, NQ] = chip_ss

        def arrived(i, carry):
            core_copy(i).wait_recv()
            return carry

        lax.fori_loop(0, HALF // 256, arrived, 0)

        def chip_copies(step, slot):
            data = remote(fwd_out.at[turn, chip_peer(step)], fwd_in.at[turn, slot], q_send.at[turn, step], q_recv.at[turn, step], chip_id(step))
            norm = remote(fwd_ss.at[turn, NQ], fwd_ss.at[turn, slot], qs_send.at[turn, step], qs_recv.at[turn, step], chip_id(step))
            return data, norm

        def give_rays(i, carry):
            step = lax.rem(i + 10, NQ)
            step = jnp.where(i >= 6, step + 1, step)
            q = chip_peer(step)
            fwd_out[turn, q] = (part_own[q] + part_in[turn, q]).astype(BF16)
            data, norm = chip_copies(step, chip)
            data.start()
            norm.start()
            return carry

        lax.fori_loop(0, NQ - 1, give_rays, 0)

        def chip_from(step):
            return lax.rem(cx + NX - step // NY, NX) * NY + lax.rem(cy + NY - lax.rem(step, NY), NY)

        def take_rays(step, total):
            slot = chip_from(step)
            data, norm = chip_copies(step, slot)
            data.wait_recv()
            norm.wait_recv()
            return total + fwd_in[turn, slot].astype(F32)

        rays_sum = lax.fori_loop(1, NQ, take_rays, part_own[chip] + part_in[turn, chip])
        total = fwd_ss[turn, 0]
        for i in range(1, NQ):
            total = total + fwd_ss[turn, i]
        alpha = jnp.sqrt(jnp.sum(total, axis=0, keepdims=True) + EPSILON)
        return rays_sum, alpha

    def chip_from(step):
        return lax.rem(cx + NX - step // NY, NX) * NY + lax.rem(cy + NY - lax.rem(step, NY), NY)

    def share_rays(turn, ray, with_data):
        if with_data:
            rays[turn, core, chip] = ray.astype(BF16)
        rays_ss[turn, chip] = squares8(ray)

        def copies(step, slot):
            both = []
            if with_data:
                both.append(remote(rays.at[turn, core, chip], rays.at[turn, core, slot], g_send.at[turn, step], g_recv.at[turn, step], chip_id(step)))
            both.append(remote(rays_ss.at[turn, chip], rays_ss.at[turn, slot], gs_send.at[turn, step], gs_recv.at[turn, step], chip_id(step)))
            return both

        def give(i, carry):
            step = lax.rem(i + 10, NQ)
            step = jnp.where(i >= 6, step + 1, step)
            for copy in copies(step, chip):
                copy.start()
            return carry

        lax.fori_loop(0, NQ - 1, give, 0)

        def take(step, carry):
            for copy in copies(step, chip_from(step)):
                copy.wait_recv()
            return carry

        lax.fori_loop(1, NQ, take, 0)
        total = rays_ss[turn, 0]
        for i in range(1, NQ):
            total = total + rays_ss[turn, i]
        half_ss[turn, 0] = total
        norm = remote(half_ss.at[turn, 0], half_ss.at[turn, 1], k_send.at[ITERS + turn], k_recv.at[ITERS + turn], other)
        norm.start()
        if with_data:
            data = remote(rays.at[turn, core], rays.at[turn, core], c_send.at[ITERS, turn], c_recv.at[ITERS, turn], other)
            back_data = remote(rays.at[turn, core], rays.at[turn, 1 - core], c_send.at[ITERS, turn], c_recv.at[ITERS, turn], other)
            data.start()
            back_data.wait_recv()
            for c in range(2):
                for i in range(HALF // 256):
                    part = rays[turn, c, i * (256 // RB) : (i + 1) * (256 // RB)].reshape(256, Z)
                    first = c * HALF + i * 256
                    rays_t[:, first : first + 256] = part.astype(F32).T.astype(BF16)
        norm.wait_recv()
        return half_ss[turn, 0] + half_ss[turn, 1]

    pl.semaphore_wait(barrier, NZ - 1 + NQ - 1 + 1)
    beta = backward(0, row_ss)
    voxel = own_back[...] / beta
    share = sino[pl.ds(pl.multiple_of(core * HALF + chip * RB, RB), RB), :]
    ray_vec = share / beta
    phi_bar = beta
    rho_bar = None
    scale = []
    steps = []
    turns = []
    for turn in range(ITERS):
        rays_sum, alpha = forward(turn, voxel)
        scale.append(alpha)
        if turn == 0:
            rho_bar = alpha
        else:
            theta = sine * alpha
            turns.append(theta / rho)
            rho_bar = -cosine * alpha
        ray_raw = rays_sum / alpha - alpha * ray_vec
        row_ss = share_rays(turn, ray_raw, turn + 1 < ITERS)
        if turn + 1 < ITERS:
            beta = backward(turn + 1, row_ss)
        else:
            last_ss[z] = row_ss

            def end_copy(step, slot):
                return remote(last_ss.at[z], last_ss.at[slot], e_send.at[step], e_recv.at[step], z_id(step))

            def give_end(step, carry):
                end_copy(step, z).start()
                return carry

            def take_end(step, carry):
                end_copy(step, z_peer(NZ - step)).wait_recv()
                return carry

            lax.fori_loop(1, NZ, give_end, 0)
            lax.fori_loop(1, NZ, take_end, 0)
            total = last_ss[0]
            for i in range(1, NZ):
                total = total + last_ss[i]
            beta = jnp.sqrt(jnp.sum(total, axis=0, keepdims=True) + EPSILON)
        rho = jnp.sqrt(rho_bar * rho_bar + beta * beta)
        cosine = rho_bar / rho
        sine = beta / rho
        phi = cosine * phi_bar
        phi_bar = sine * phi_bar
        steps.append(phi / rho)
        if turn + 1 < ITERS:
            ray_vec = ray_raw / beta
            voxel = own_back[...] / beta - beta * (voxel / alpha)

    residual[...] = phi_bar
    part = [None] * ITERS
    weight = steps[-1]
    for k in reversed(range(ITERS)):
        part[k] = weight / scale[k]
        if k:
            weight = steps[k - 1] - weight * turns[k - 1]

    def low_wait(turn):
        def take(step, carry):
            slot = z_peer(NZ - step)
            remote(low.at[turn, z], low.at[turn, slot], l_send.at[turn, step], l_recv.at[turn, step], z_id(step)).wait_recv()
            return carry

        lax.fori_loop(1, NZ, take, 0)

    for turn in range(ITERS):
        low_wait(turn)

    def combine(p, carry):
        total = None
        for k in range(ITERS):
            term = part[k] * (high[k, p].astype(F32) + low[k, p].astype(F32))
            total = term if total is None else total + term
        out[pl.ds(pl.multiple_of(p * VB, VB), VB), :] = total
        return carry

    lax.fori_loop(0, NZ, combine, 0)

    def sent_z(step, carry):
        for turn in range(ITERS):
            p = z_peer(step)
            remote(quant.at[turn, p], back.at[turn, z], z_send.at[turn, step], z_recv.at[turn, step], z_id(step)).wait_send()
            remote(quant_meta.at[turn, p], back_meta.at[turn, z], zm_send.at[turn, step], zm_recv.at[turn, step], z_id(step)).wait_send()
            remote(high.at[turn, z], high.at[turn, z], h_send.at[turn, step], h_recv.at[turn, step], z_id(step)).wait_send()
            remote(high_ss.at[turn, z], high_ss.at[turn, z], hs_send.at[turn, step], hs_recv.at[turn, step], z_id(step)).wait_send()
            remote(low.at[turn, z], low.at[turn, z], l_send.at[turn, step], l_recv.at[turn, step], z_id(step)).wait_send()
        remote(last_ss.at[z], last_ss.at[z], e_send.at[step], e_recv.at[step], z_id(step)).wait_send()
        return carry

    lax.fori_loop(1, NZ, sent_z, 0)

    def sent_chip(step, carry):
        q = chip_peer(step)
        for turn in range(ITERS):
            remote(fwd_out.at[turn, q], fwd_in.at[turn, chip], q_send.at[turn, step], q_recv.at[turn, step], chip_id(step)).wait_send()
            remote(fwd_ss.at[turn, NQ], fwd_ss.at[turn, chip], qs_send.at[turn, step], qs_recv.at[turn, step], chip_id(step)).wait_send()
            remote(rays_ss.at[turn, chip], rays_ss.at[turn, chip], gs_send.at[turn, step], gs_recv.at[turn, step], chip_id(step)).wait_send()
            if turn + 1 < ITERS:
                remote(
                    rays.at[turn, core, chip], rays.at[turn, core, chip], g_send.at[turn, step], g_recv.at[turn, step], chip_id(step)
                ).wait_send()
        return carry

    lax.fori_loop(1, NQ, sent_chip, 0)

    for turn in range(ITERS):
        remote(part_ss.at[turn, 0], part_ss.at[turn, 1], k_send.at[turn], k_recv.at[turn], other).wait_send()
        remote(half_ss.at[turn, 0], half_ss.at[turn, 1], k_send.at[ITERS + turn], k_recv.at[ITERS + turn], other).wait_send()
        for i in range(HALF // 256):
            at = pl.ds(i * (256 // RB), 256 // RB)
            remote(part_out.at[turn, at], part_in.at[turn, at], c_send.at[turn, i], c_recv.at[turn, i], other).wait_send()
        if turn + 1 < ITERS:
            remote(rays.at[turn, core], rays.at[turn, core], c_send.at[ITERS, turn], c_recv.at[ITERS, turn], other).wait_send()


def body(tile_values, tile_rows, tile_cols, tile_count, sinogram):
    values = tile_values[0, 0]
    place = tile_rows[0, 0] * (BLK // TILE) + tile_cols[0, 0]
    slots = jnp.arange(place.shape[0], dtype=jnp.int32)
    live = slots < tile_count[0, 0]
    targets = jnp.arange((BLK // TILE) ** 2, dtype=jnp.int32)
    here = (place[None, :] == targets[:, None]) & live[None, :]
    inv = jnp.max(jnp.where(here, slots[None, :], -1), axis=1)
    dma = pltpu.SemaphoreType.DMA
    vmem = pltpu.VMEM
    scratch = [
        vmem((NZ, BLK, VB), BF16),
        vmem((Z, BLK), BF16),
        vmem((ITERS, NZ, VB, Z), jnp.int16),
        vmem((ITERS, NZ, 16, Z), F32),
        vmem((ITERS, NZ, VB, Z), jnp.int16),
        vmem((ITERS, NZ, 16, Z), F32),
        vmem((VB, Z), F32),
        vmem((ITERS, NZ, VB, Z), BF16),
        vmem((ITERS, NZ, VB, Z), BF16),
        vmem((ITERS, NZ, 8, Z), F32),
        vmem((NQ, RB, Z), F32),
        vmem((ITERS, NQ, RB, Z), F32),
        vmem((ITERS, NQ, RB, Z), F32),
        vmem((ITERS, 2, 8, Z), F32),
        vmem((ITERS, NQ, RB, Z), BF16),
        vmem((ITERS, NQ, RB, Z), BF16),
        vmem((ITERS, NQ + 1, 8, Z), F32),
        vmem((ITERS - 1, 2, NQ, RB, Z), BF16),
        vmem((ITERS, NQ, 8, Z), F32),
        vmem((ITERS, 2, 8, Z), F32),
        vmem((NZ, 8, Z), F32),
    ]
    for shape in (
        (ITERS, NZ),
        (ITERS, NZ),
        (ITERS, NZ),
        (ITERS, NZ),
        (ITERS, NZ),
        (ITERS + 1, HALF // 256),
        (ITERS, NQ),
        (ITERS, NQ),
        (ITERS, NQ),
        (ITERS, NQ),
        (2 * ITERS,),
        (NZ,),
    ):
        scratch += [dma(shape), dma(shape)]
    found, residual = pl.pallas_call(
        kernel,
        out_shape=(jax.ShapeDtypeStruct((BLK, Z), F32), jax.ShapeDtypeStruct((1, Z), F32)),
        in_specs=[
            pl.BlockSpec(memory_space=pltpu.SMEM),
            pl.BlockSpec(memory_space=pltpu.VMEM),
            pl.BlockSpec(memory_space=pltpu.VMEM),
        ],
        out_specs=(pl.BlockSpec(memory_space=pltpu.VMEM), pl.BlockSpec(memory_space=pltpu.VMEM)),
        scratch_shapes=scratch,
        compiler_params=pltpu.CompilerParams(collective_id=0, has_side_effects=True, vmem_limit_bytes=60 * 1024 * 1024),
    )(inv, values, sinogram)
    return found, residual[0]


def solution(mesh):
    split = Mesh(mesh.devices.reshape(NZ, NX, NY, 2), ("row", "cx", "cy", "cc"))
    col = ("cx", "cy", "cc")
    placed = (
        P("row", col, None, None, None),
        P("row", col, None),
        P("row", col, None),
        P("row", col),
        P("row", None),
    )
    return jax.shard_map(body, mesh=split, in_specs=placed, out_specs=(P(col, None), P()), check_vma=False)
```

```python
import jax
import jax.numpy as jnp
from jax import lax
from jax.experimental import pallas as pl
from jax.experimental.pallas import tpu as pltpu
from jax.sharding import Mesh
from jax.sharding import PartitionSpec as P

ITERS = 3
NZ = 8
NX = 4
NY = 4
NQ = NX * NY
TILE = 128
Z = 128
BLK = 2048
VB = BLK // NZ
HV = VB // 2
HALF = BLK // 2
RB = HALF // NQ
CB = 256 // RB
EPSILON = 1e-06
MESH = pl.DeviceIdType.MESH
F32 = jnp.float32
BF16 = jnp.bfloat16


def looped(name, first, last, step, carry):
    with jax.named_scope(name):
        return lax.fori_loop(first, last, step, carry)


def squares(x):
    return jnp.sum(x * x, axis=0, keepdims=True)


def sum_rows(ref, turn, count):
    total = ref[turn, 0]
    for i in range(1, count):
        total = total + ref[turn, i]
    return total


GATHER = (
    (2, 0, 0),
    (-2, 0, 1),
    (2, 0, 1),
    (-2, 0, 0),
    (1, 0, None),
    (-1, 0, None),
    (2, -2, 0),
    (-2, 2, 1),
    (1, -2, 0),
    (-1, 2, 1),
    (1, -2, 1),
    (-1, 2, 0),
)
REDUCE = (
    (1, 0, 1),
    (1, 1, 1),
    (-1, 2, 1),
    (-1, 3, 1),
    (2, 4, 1),
    (-2, 5, 1),
    (1, 6, 2),
    (-1, 8, 2),
    (2, 10, 1),
    (2, 11, 1),
    (-2, 12, 1),
    (-2, 13, 1),
)
UNITS = 14


def kernel(
    inv,
    values_hbm,
    sino_hbm,
    done,
    last,
    rows,
    values,
    sino,
    dense,
    rays_t,
    quant,
    quant_scale,
    back,
    back_scale,
    row_ss,
    relay,
    own_back,
    high,
    low,
    high_ss,
    part_own,
    part_out,
    part_in,
    part_ss,
    fwd_out,
    fwd_in,
    fwd_ss,
    rays,
    rays_ss,
    half_ss,
    in_sem,
    z_send,
    z_recv,
    zm_send,
    zm_recv,
    zs_send,
    zs_recv,
    h_send,
    h_recv,
    hs_send,
    hs_recv,
    l_send,
    l_recv,
    c_send,
    c_recv,
    q_send,
    q_recv,
    qs_send,
    qs_recv,
    g_send,
    g_recv,
    gs_send,
    gs_recv,
    k_send,
    k_recv,
):
    z = lax.axis_index("row")
    cx = lax.axis_index("cx")
    cy = lax.axis_index("cy")
    core = lax.axis_index("cc")
    chip = cx * NY + cy

    def z_at(step):
        return lax.rem(z + (step + NZ), NZ)

    def z_id(step):
        return {"row": z_at(step)}

    def chip_at(step):
        return lax.rem(cx + step // NY, NX), lax.rem(cy + lax.rem(step, NY), NY)

    def chip_id(step):
        px, py = chip_at(step)
        return {"cx": px, "cy": py}

    def chip_peer(step):
        px, py = chip_at(step)
        return px * NY + py

    def chip_from(step):
        return lax.rem(cx + NX - step // NY, NX) * NY + lax.rem(cy + NY - lax.rem(step, NY), NY)

    other = {"cc": 1 - core}

    barrier = pltpu.get_barrier_semaphore()

    def greet_z(step, carry):
        pl.semaphore_signal(barrier, inc=1, device_id=z_id(step), device_id_type=MESH)
        return carry

    def greet_chip(step, carry):
        pl.semaphore_signal(barrier, inc=1, device_id=chip_id(step), device_id_type=MESH)
        return carry

    looped("greet_z", 1, NZ, greet_z, 0)
    looped("greet_chip", 1, NQ, greet_chip, 0)
    pl.semaphore_signal(barrier, inc=1, device_id=other, device_id_type=MESH)

    sino_copy = pltpu.make_async_copy(sino_hbm, sino, in_sem.at[0])
    values_copy = pltpu.make_async_copy(values_hbm, values, in_sem.at[1])
    sino_copy.start()
    values_copy.start()

    def remote(src, dst, send, recv, device):
        return pltpu.make_async_remote_copy(
            src_ref=src, dst_ref=dst, send_sem=send, recv_sem=recv, device_id=device, device_id_type=MESH
        )

    def read_sino(i, total):
        at = pl.ds(pl.multiple_of(i * 256, 256), 256)
        block = sino[at, :]
        rays_t[:, at] = block.T.astype(BF16)
        return total + jnp.sum((block * block).reshape(-1, 8, Z), axis=0)

    def fill(i, carry):
        at = pl.ds(pl.multiple_of(i * TILE, TILE), TILE)
        for j in range(BLK // TILE):
            slot = inv[i * (BLK // TILE) + j]
            tile = values[jnp.maximum(slot, 0)]
            tile = jnp.where(slot >= 0, tile, jnp.zeros_like(tile))
            dense[j // 2, at, (j % 2) * TILE : (j % 2 + 1) * TILE] = tile
        return carry

    with jax.named_scope("sino_in"):
        sino_copy.wait()
    first_ss = looped("read_sino", 0, BLK // 256, read_sino, jnp.zeros((8, Z), F32))
    with jax.named_scope("values_in"):
        values_copy.wait()
    looped("fill", 0, BLK // TILE, fill, 0)

    def row_copy(turn, step, slot):
        return remote(row_ss.at[turn, z], row_ss.at[turn, slot], zs_send.at[turn, step], zs_recv.at[turn, step], z_id(step))

    def give_norm(turn, total):
        row_ss[turn, z] = total

        def give(step, carry):
            row_copy(turn, step, z).start()
            return carry

        looped("give_norm", 1, NZ, give, 0)

    def take_norm(turn):
        def take(step, carry):
            row_copy(turn, step, z_at(-step)).wait_recv()
            return carry

        looped("take_norm", 1, NZ, take, 0)
        return jnp.sqrt(sum_rows(row_ss, turn, NZ) + EPSILON)

    def reduce_copies(turn, message):
        step, unit, units = message
        at = pl.ds(unit, units)
        data = remote(quant.at[turn, at], back.at[turn, at], z_send.at[turn, unit], z_recv.at[turn, unit], z_id(step))
        scale = remote(
            quant_scale.at[turn, at], back_scale.at[turn, at], zm_send.at[turn, unit], zm_recv.at[turn, unit], z_id(step)
        )
        return data, scale

    def send_units(turn, *units):
        for message in REDUCE:
            if message[1] in units:
                for copy in reduce_copies(turn, message):
                    copy.start()

    def await_units(turn, *units):
        for message in REDUCE:
            if message[1] in units:
                for copy in reduce_copies(turn, message):
                    copy.wait_recv()

    def pack(turn, unit, block):
        top = jnp.maximum(jnp.max(jnp.abs(block), axis=0, keepdims=True), 1e-30)
        quant[turn, unit] = jnp.round(block * (32767.0 / top)).astype(jnp.int32).astype(jnp.int16)
        quant_scale[turn, unit] = top * (1.0 / 32767.0)

    def unpack(turn, unit):
        return back[turn, unit].astype(jnp.int32).astype(F32) * back_scale[turn, unit]

    def product(p):
        return jnp.dot(rays_t[...], dense[p], preferred_element_type=F32)

    def backward(turn):
        with jax.named_scope("give_4"):
            block = product(z_at(4))
            pack(turn, 4, block[:, :HV].T)
            pack(turn, 5, block[:, HV:].T)
            send_units(turn, 4, 5)
        for step, unit in ((3, 0), (-3, 2)):
            with jax.named_scope("give_3"):
                block = product(z_at(step))
                pack(turn, unit, block[:, :HV].T)
                pack(turn, unit + 1, block[:, HV:].T)
                send_units(turn, unit, unit + 1)
        for step, unit in ((1, 6), (-1, 8)):
            with jax.named_scope("give_1"):
                block = product(z_at(step))
                pack(turn, unit, block[:, :HV].T)
                pack(turn, unit + 1, block[:, HV:].T)
                send_units(turn, unit)
        for i, step in enumerate((2, -2)):
            with jax.named_scope("make_2"):
                block = product(z_at(step))
                relay[2 * i] = block[:, :HV].T
                relay[2 * i + 1] = block[:, HV:].T
        with jax.named_scope("make_0"):
            block = product(z)
            own_back[:HV] = block[:, :HV].T
            own_back[HV:] = block[:, HV:].T
        with jax.named_scope("relay_wait"):
            await_units(turn, 0, 4)
        with jax.named_scope("relay"):
            pack(turn, 10, relay[0] + unpack(turn, 0) + unpack(turn, 4))
            send_units(turn, 10)
        with jax.named_scope("relay_wait"):
            await_units(turn, 3, 5)
        with jax.named_scope("relay"):
            pack(turn, 13, relay[3] + unpack(turn, 3) + unpack(turn, 5))
            send_units(turn, 13)
        with jax.named_scope("relay_wait"):
            await_units(turn, 1)
        with jax.named_scope("relay"):
            pack(turn, 11, relay[1] + unpack(turn, 1))
            send_units(turn, 11)
        with jax.named_scope("relay_wait"):
            await_units(turn, 2)
        with jax.named_scope("relay"):
            pack(turn, 12, relay[2] + unpack(turn, 2))
            send_units(turn, 12)
        beta = take_norm(turn)
        with jax.named_scope("reduce_1"):
            await_units(turn, 6, 8)
            own_back[:HV] += unpack(turn, 6) + unpack(turn, 8)
            own_back[HV:] += unpack(turn, 7) + unpack(turn, 9)
        with jax.named_scope("reduce_2"):
            await_units(turn, 10, 13)
            await_units(turn, 11, 12)
        with jax.named_scope("reduce_3"):
            own_back[:HV] += unpack(turn, 10) + unpack(turn, 12)
            own_back[HV:] += unpack(turn, 11) + unpack(turn, 13)
        return beta

    def gather_copy(turn, k, receiving):
        step, block, half = GATHER[k]
        slot = z_at(block - step if receiving else block)
        rows_at = pl.ds(0, VB) if half is None else pl.ds(half * HV, HV)
        view = high.at[turn, slot, rows_at]
        return remote(view, view, h_send.at[turn, k], h_recv.at[turn, k], z_id(step))

    def high_norm(turn, step, slot):
        return remote(high_ss.at[turn, z], high_ss.at[turn, slot], hs_send.at[turn, step], hs_recv.at[turn, step], z_id(step))

    def low_copy(turn, step, slot):
        return remote(low.at[turn, z], low.at[turn, slot], l_send.at[turn, step], l_recv.at[turn, step], z_id(step))

    def forward(turn, voxel):
        with jax.named_scope("gather"):
            top = voxel.astype(BF16)
            high[turn, z] = top
            for k in range(6):
                gather_copy(turn, k, False).start()
            low[turn, z] = (voxel - top.astype(F32)).astype(BF16)
            high_ss[turn, z] = squares(voxel)

        def give(step, carry):
            high_norm(turn, step, z).start()
            return carry

        looped("give_norm", 1, NZ, give, 0)
        for arrived, onward in ((0, (6, 8)), (1, (7, 9)), (2, (10,)), (3, (11,))):
            with jax.named_scope("gather_relay"):
                gather_copy(turn, arrived, True).wait_recv()
                for k in onward:
                    gather_copy(turn, k, False).start()
        with jax.named_scope("gather_1"):
            gather_copy(turn, 4, True).wait_recv()
            gather_copy(turn, 5, True).wait_recv()

        def product(at, steps):
            block = None
            for step in steps:
                p = z_at(step)
                term = jnp.dot(dense[p, at, :], high[turn, p], preferred_element_type=F32)
                block = term if block is None else block + term
            return block.reshape(CB, RB, Z)

        near = (0, 1, -1, 2, -2)
        far = (3, -3, 4)

        def theirs_at(i):
            return pl.ds(pl.multiple_of((1 - core) * HALF + i * 256, 256), 256)

        def ours_at(i):
            return pl.ds(pl.multiple_of(core * HALF + i * 256, 256), 256)

        def near_product(i, carry):
            at = pl.ds(i * CB, CB)
            part_out[turn, at] = product(theirs_at(i), near)
            part_own[at] = product(ours_at(i), near)
            return carry

        looped("near_product", 0, HALF // 256, near_product, 0)
        with jax.named_scope("gather_3"):
            for k in (8, 9, 10, 11, 6, 7):
                gather_copy(turn, k, True).wait_recv()

        def give_low(step, carry):
            low_copy(turn, step, z).start()
            return carry

        def core_copy(i):
            at = pl.ds(i * CB, CB)
            return remote(part_out.at[turn, at], part_in.at[turn, at], c_send.at[turn, i], c_recv.at[turn, i], other)

        def theirs(i, carry):
            at = pl.ds(i * CB, CB)
            part_out[turn, at] += product(theirs_at(i), far)
            core_copy(i).start()
            return carry

        looped("theirs", 0, HALF // 256, theirs, 0)

        def take(step, carry):
            high_norm(turn, step, z_at(-step)).wait_recv()
            return carry

        looped("take_norm", 1, NZ, take, 0)
        part_ss[turn, 0] = sum_rows(high_ss, turn, NZ)
        core_norm = remote(part_ss.at[turn, 0], part_ss.at[turn, 1], k_send.at[turn], k_recv.at[turn], other)
        core_norm.start()

        def ours(i, carry):
            part_own[pl.ds(i * CB, CB)] += product(ours_at(i), far)
            return carry

        looped("ours", 0, HALF // 256, ours, 0)
        with jax.named_scope("core_wait"):
            core_norm.wait_recv()
            chip_ss = part_ss[turn, 0] + part_ss[turn, 1]
            fwd_ss[turn, chip] = chip_ss
            fwd_ss[turn, NQ] = chip_ss
            for i in range(HALF // 256):
                core_copy(i).wait_recv()

        def chip_copies(step, slot):
            data = remote(
                fwd_out.at[turn, chip_peer(step)], fwd_in.at[turn, slot], q_send.at[turn, step], q_recv.at[turn, step], chip_id(step)
            )
            norm = remote(fwd_ss.at[turn, NQ], fwd_ss.at[turn, slot], qs_send.at[turn, step], qs_recv.at[turn, step], chip_id(step))
            return data, norm

        def give_rays(i, carry):
            step = lax.rem(i + 10, NQ)
            step = jnp.where(i >= 6, step + 1, step)
            q = chip_peer(step)
            fwd_out[turn, q] = (part_own[q] + part_in[turn, q]).astype(BF16)
            data, norm = chip_copies(step, chip)
            data.start()
            norm.start()
            return carry

        looped("give_rays", 0, NQ - 1, give_rays, 0)
        looped("give_low", 1, NZ, give_low, 0)

        def take_rays(step, total):
            slot = chip_from(step)
            data, norm = chip_copies(step, slot)
            data.wait_recv()
            norm.wait_recv()
            return total + fwd_in[turn, slot].astype(F32)

        rays_sum = looped("take_rays", 1, NQ, take_rays, part_own[chip] + part_in[turn, chip])
        alpha = jnp.sqrt(sum_rows(fwd_ss, turn, NQ) + EPSILON)
        return rays_sum, alpha

    def share_rays(turn, ray, with_data):
        if with_data:
            rays[turn, core, chip] = ray.astype(BF16)
        rays_ss[turn, chip] = squares(ray)

        def copies(step, slot):
            both = []
            if with_data:
                both.append(
                    remote(
                        rays.at[turn, core, chip],
                        rays.at[turn, core, slot],
                        g_send.at[turn, step],
                        g_recv.at[turn, step],
                        chip_id(step),
                    )
                )
            both.append(
                remote(rays_ss.at[turn, chip], rays_ss.at[turn, slot], gs_send.at[turn, step], gs_recv.at[turn, step], chip_id(step))
            )
            return both

        def give(i, carry):
            step = lax.rem(i + 10, NQ)
            step = jnp.where(i >= 6, step + 1, step)
            for copy in copies(step, chip):
                copy.start()
            return carry

        looped("share", 0, NQ - 1, give, 0)

        def take(step, carry):
            for copy in copies(step, chip_from(step)):
                copy.wait_recv()
            return carry

        looped("take_share", 1, NQ, take, 0)
        half_ss[turn, 0] = sum_rows(rays_ss, turn, NQ)
        norm = remote(half_ss.at[turn, 0], half_ss.at[turn, 1], k_send.at[ITERS + turn], k_recv.at[ITERS + turn], other)
        norm.start()
        if with_data:
            data = remote(rays.at[turn, core], rays.at[turn, core], c_send.at[ITERS, turn], c_recv.at[ITERS, turn], other)
            back_data = remote(rays.at[turn, core], rays.at[turn, 1 - core], c_send.at[ITERS, turn], c_recv.at[ITERS, turn], other)
            data.start()

            def turned(c):
                for i in range(HALF // 256):
                    part = rays[turn, c, i * CB : (i + 1) * CB].reshape(256, Z)
                    first = pl.multiple_of(c * HALF + i * 256, 256)
                    rays_t[:, pl.ds(first, 256)] = part.astype(F32).T.astype(BF16)

            turned(core)
            with jax.named_scope("core_rays"):
                back_data.wait_recv()
            turned(1 - core)
        norm.wait_recv()
        return half_ss[turn, 0] + half_ss[turn, 1]

    with jax.named_scope("barrier"):
        pl.semaphore_wait(barrier, NZ - 1 + NQ - 1 + 1)
    give_norm(0, jnp.sum(first_ss, axis=0, keepdims=True))
    beta = backward(0)
    voxel = own_back[...] / beta
    share = sino[pl.ds(pl.multiple_of(core * HALF + chip * RB, RB), RB), :]
    ray_vec = share / beta
    phi_bar = beta
    rho_bar = None
    scale = []
    steps = []
    turns = []
    for turn in range(ITERS):
        rays_sum, alpha = forward(turn, voxel)
        scale.append(alpha)
        if turn == 0:
            rho_bar = alpha
        else:
            theta = sine * alpha
            turns.append(theta / rho)
            rho_bar = -cosine * alpha
        ray_raw = rays_sum / alpha - alpha * ray_vec
        give_norm(turn + 1, share_rays(turn, ray_raw, turn + 1 < ITERS))
        if turn + 1 < ITERS:
            beta = backward(turn + 1)
            rho = jnp.sqrt(rho_bar * rho_bar + beta * beta)
            cosine = rho_bar / rho
            sine = beta / rho
            phi = cosine * phi_bar
            phi_bar = sine * phi_bar
            steps.append(phi / rho)
            ray_vec = ray_raw / beta
            voxel = own_back[...] / beta - beta * (voxel / alpha)

    weight = [[None] * ITERS for _ in range(ITERS)]
    for k in range(ITERS):
        weight[k][k] = 1.0 / scale[k]
        for j in range(k):
            weight[k][j] = -turns[k - 1] * weight[k - 1][j]
    known = [steps[0] * weight[0][0] + steps[1] * weight[1][0], steps[1] * weight[1][1]]
    final = weight[ITERS - 1]

    for turn in range(ITERS):

        def take_low(step, carry):
            low_copy(turn, step, z_at(-step)).wait_recv()
            return carry

        looped("take_low", 1, NZ, take_low, 0)

    def combine(p, carry):
        at = pl.ds(pl.multiple_of(p * VB, VB), VB)
        base = step = None
        for k in range(ITERS):
            value = high[k, p].astype(F32) + low[k, p].astype(F32)
            step = final[k] * value if step is None else step + final[k] * value
            if k < len(known):
                base = known[k] * value if base is None else base + known[k] * value
        done[at, :] = base
        last[at, :] = step
        return carry

    looped("combine", 0, NZ, combine, 0)
    beta = take_norm(ITERS)
    rho = jnp.sqrt(rho_bar * rho_bar + beta * beta)
    cosine = rho_bar / rho
    sine = beta / rho
    rows[0:1, :] = (cosine * phi_bar) / rho
    rows[1:2, :] = sine * phi_bar

    def sent_z(step, carry):
        for turn in range(ITERS):
            high_norm(turn, step, z).wait_send()
            low_copy(turn, step, z).wait_send()
        for turn in range(ITERS + 1):
            row_copy(turn, step, z).wait_send()
        return carry

    looped("sent_z", 1, NZ, sent_z, 0)
    for turn in range(ITERS):
        for message in REDUCE:
            for copy in reduce_copies(turn, message):
                copy.wait_send()
        for k in range(len(GATHER)):
            gather_copy(turn, k, False).wait_send()

    def sent_chip(step, carry):
        q = chip_peer(step)
        for turn in range(ITERS):
            remote(fwd_out.at[turn, q], fwd_in.at[turn, chip], q_send.at[turn, step], q_recv.at[turn, step], chip_id(step)).wait_send()
            remote(fwd_ss.at[turn, NQ], fwd_ss.at[turn, chip], qs_send.at[turn, step], qs_recv.at[turn, step], chip_id(step)).wait_send()
            remote(rays_ss.at[turn, chip], rays_ss.at[turn, chip], gs_send.at[turn, step], gs_recv.at[turn, step], chip_id(step)).wait_send()
            if turn + 1 < ITERS:
                remote(
                    rays.at[turn, core, chip], rays.at[turn, core, chip], g_send.at[turn, step], g_recv.at[turn, step], chip_id(step)
                ).wait_send()
        return carry

    looped("sent_chip", 1, NQ, sent_chip, 0)

    for turn in range(ITERS):
        remote(part_ss.at[turn, 0], part_ss.at[turn, 1], k_send.at[turn], k_recv.at[turn], other).wait_send()
        remote(half_ss.at[turn, 0], half_ss.at[turn, 1], k_send.at[ITERS + turn], k_recv.at[ITERS + turn], other).wait_send()
        for i in range(HALF // 256):
            at = pl.ds(i * CB, CB)
            remote(part_out.at[turn, at], part_in.at[turn, at], c_send.at[turn, i], c_recv.at[turn, i], other).wait_send()
        if turn + 1 < ITERS:
            remote(rays.at[turn, core], rays.at[turn, core], c_send.at[ITERS, turn], c_recv.at[ITERS, turn], other).wait_send()


def finish(done, last, rows, out, residual):
    out[...] = done[...] + rows[0:1, :] * last[...]
    residual[...] = rows[1:2, :]


def body(tile_values, tile_rows, tile_cols, tile_count, sinogram):
    values = tile_values[0, 0]
    slots = jnp.arange(tile_rows.shape[-1], dtype=jnp.int32)[None, :]
    targets = jnp.arange((BLK // TILE) ** 2, dtype=jnp.int32)[:, None]
    here = (tile_rows[0] == targets // (BLK // TILE)) & (tile_cols[0] == targets % (BLK // TILE)) & (slots < tile_count)
    inv = jnp.max(jnp.where(here, slots, -1), axis=1)
    dma = pltpu.SemaphoreType.DMA
    vmem = pltpu.VMEM
    tiles = values.shape
    scratch = [
        vmem(tiles, BF16),
        vmem((BLK, Z), F32),
        vmem((NZ, BLK, VB), BF16),
        vmem((Z, BLK), BF16),
        vmem((ITERS, UNITS, HV, Z), jnp.int16),
        vmem((ITERS, UNITS, 1, Z), F32),
        vmem((ITERS, UNITS, HV, Z), jnp.int16),
        vmem((ITERS, UNITS, 1, Z), F32),
        vmem((ITERS + 1, NZ, 1, Z), F32),
        vmem((4, HV, Z), F32),
        vmem((VB, Z), F32),
        vmem((ITERS, NZ, VB, Z), BF16),
        vmem((ITERS, NZ, VB, Z), BF16),
        vmem((ITERS, NZ, 1, Z), F32),
        vmem((NQ, RB, Z), F32),
        vmem((ITERS, NQ, RB, Z), F32),
        vmem((ITERS, NQ, RB, Z), F32),
        vmem((ITERS, 2, 1, Z), F32),
        vmem((ITERS, NQ, RB, Z), BF16),
        vmem((ITERS, NQ, RB, Z), BF16),
        vmem((ITERS, NQ + 1, 1, Z), F32),
        vmem((ITERS - 1, 2, NQ, RB, Z), BF16),
        vmem((ITERS, NQ, 1, Z), F32),
        vmem((ITERS, 2, 1, Z), F32),
        dma((2,)),
    ]
    for shape in (
        (ITERS, UNITS),
        (ITERS, UNITS),
        (ITERS + 1, NZ),
        (ITERS, len(GATHER)),
        (ITERS, NZ),
        (ITERS, NZ),
        (ITERS + 1, HALF // 256),
        (ITERS, NQ),
        (ITERS, NQ),
        (ITERS, NQ),
        (ITERS, NQ),
        (2 * ITERS,),
    ):
        scratch += [dma(shape), dma(shape)]
    in_vmem = pl.BlockSpec(memory_space=pltpu.VMEM)
    block = jax.ShapeDtypeStruct((BLK, Z), F32)
    done, last, rows = pl.pallas_call(
        kernel,
        out_shape=(block, block, jax.ShapeDtypeStruct((8, Z), F32)),
        in_specs=[
            pl.BlockSpec(memory_space=pltpu.SMEM),
            pl.BlockSpec(memory_space=pl.ANY),
            pl.BlockSpec(memory_space=pl.ANY),
        ],
        out_specs=(in_vmem, in_vmem, in_vmem),
        scratch_shapes=scratch,
        compiler_params=pltpu.CompilerParams(collective_id=0, has_side_effects=True, vmem_limit_bytes=48 * 1024 * 1024),
    )(inv, values, sinogram)
    found, residual = pl.pallas_call(
        finish,
        out_shape=(block, jax.ShapeDtypeStruct((1, Z), F32)),
        in_specs=[in_vmem, in_vmem, in_vmem],
        out_specs=(in_vmem, in_vmem),
        compiler_params=pltpu.CompilerParams(vmem_limit_bytes=8 * 1024 * 1024),
    )(done, last, rows)
    return found, residual[0]


def solution(mesh):
    split = Mesh(mesh.devices.reshape(NZ, NX, NY, 2), ("row", "cx", "cy", "cc"))
    col = ("cx", "cy", "cc")
    placed = (
        P("row", col, None, None, None),
        P("row", col, None),
        P("row", col, None),
        P("row", col),
        P("row", None),
    )
    return jax.shard_map(body, mesh=split, in_specs=placed, out_specs=(P(col, None), P()), check_vma=False)
```

```python
import jax
import jax.numpy as jnp
from jax import lax
from jax.experimental import pallas as pl
from jax.experimental.pallas import tpu as pltpu
from jax.sharding import Mesh
from jax.sharding import PartitionSpec as P

ITERS = 3
NZ = 8
NX = 4
NY = 4
NQ = NX * NY
TILE = 128
Z = 128
BLK = 2048
VB = BLK // NZ
HV = VB // 2
HALF = BLK // 2
RB = HALF // NQ
CB = 256 // RB
EPSILON = 1e-06
MESH = pl.DeviceIdType.MESH
F32 = jnp.float32
BF16 = jnp.bfloat16


def looped(name, first, last, step, carry):
    with jax.named_scope(name):
        return lax.fori_loop(first, last, step, carry)


def squares(x):
    return jnp.sum(x * x, axis=0, keepdims=True)


def sum_rows(ref, turn, count):
    total = ref[turn, 0]
    for i in range(1, count):
        total = total + ref[turn, i]
    return total


GATHER = (
    (2, 0, 0),
    (-2, 0, 1),
    (2, 0, 1),
    (-2, 0, 0),
    (1, 0, None),
    (-1, 0, None),
    (2, -2, 0),
    (-2, 2, 1),
    (1, -2, 0),
    (-1, 2, 1),
    (1, -2, 1),
    (-1, 2, 0),
)
REDUCE = (
    (1, 0, 1),
    (1, 1, 1),
    (-1, 2, 1),
    (-1, 3, 1),
    (2, 4, 1),
    (-2, 5, 1),
    (1, 6, 2),
    (-1, 8, 2),
    (2, 10, 1),
    (2, 11, 1),
    (-2, 12, 1),
    (-2, 13, 1),
)
UNITS = 14
CHIPS = sorted(range(1, NQ), key=lambda step: -(min(step // NY, NX - step // NY) + min(step % NY, NY - step % NY)))


def kernel(
    inv,
    values_hbm,
    sino_hbm,
    done,
    last,
    rows,
    values,
    sino,
    dense,
    rays_t,
    quant,
    quant_scale,
    back,
    back_scale,
    row_ss,
    relay,
    own_back,
    high,
    low,
    high_ss,
    part_own,
    part_out,
    part_in,
    part_ss,
    fwd_out,
    fwd_in,
    fwd_ss,
    rays,
    rays_ss,
    half_ss,
    last_ss,
    in_sem,
    z_send,
    z_recv,
    zm_send,
    zm_recv,
    zs_send,
    zs_recv,
    h_send,
    h_recv,
    hs_send,
    hs_recv,
    l_send,
    l_recv,
    c_send,
    c_recv,
    q_send,
    q_recv,
    qs_send,
    qs_recv,
    g_send,
    g_recv,
    gs_send,
    gs_recv,
    k_send,
    k_recv,
    n_send,
    n_recv,
    r_send,
    r_recv,
    e_send,
    e_recv,
):
    z = lax.axis_index("row")
    cx = lax.axis_index("cx")
    cy = lax.axis_index("cy")
    core = lax.axis_index("cc")
    chip = cx * NY + cy

    def z_at(step):
        return lax.rem(z + (step + NZ), NZ)

    def z_id(step):
        return {"row": z_at(step)}

    def across_id(step):
        return {"row": z_at(step), "cc": 1 - core}

    def chip_at(step):
        return lax.rem(cx + step // NY, NX), lax.rem(cy + lax.rem(step, NY), NY)

    def chip_id(step):
        px, py = chip_at(step)
        return {"cx": px, "cy": py}

    def chip_peer(step):
        px, py = chip_at(step)
        return px * NY + py

    def chip_from(step):
        return lax.rem(cx + NX - step // NY, NX) * NY + lax.rem(cy + NY - lax.rem(step, NY), NY)

    other = {"cc": 1 - core}

    barrier = pltpu.get_barrier_semaphore()

    def greet_z(step, carry):
        pl.semaphore_signal(barrier, inc=1, device_id=z_id(step), device_id_type=MESH)
        return carry

    def greet_chip(step, carry):
        pl.semaphore_signal(barrier, inc=1, device_id=chip_id(step), device_id_type=MESH)
        return carry

    def greet_across(step, carry):
        pl.semaphore_signal(barrier, inc=1, device_id=across_id(step), device_id_type=MESH)
        return carry

    looped("greet_z", 1, NZ, greet_z, 0)
    looped("greet_across", 1, NZ, greet_across, 0)
    looped("greet_chip", 1, NQ, greet_chip, 0)
    pl.semaphore_signal(barrier, inc=1, device_id=other, device_id_type=MESH)

    sino_copy = pltpu.make_async_copy(sino_hbm, sino, in_sem.at[0])
    values_copy = pltpu.make_async_copy(values_hbm, values, in_sem.at[1])
    sino_copy.start()
    values_copy.start()

    def remote(src, dst, send, recv, device):
        return pltpu.make_async_remote_copy(
            src_ref=src, dst_ref=dst, send_sem=send, recv_sem=recv, device_id=device, device_id_type=MESH
        )

    def took(view, sem):
        remote(view, view, sem, sem, other).wait_recv()

    def left(view, sem):
        remote(view, view, sem, sem, other).wait_send()

    def read_sino(i, total):
        at = pl.ds(pl.multiple_of(i * 256, 256), 256)
        block = sino[at, :]
        rays_t[:, at] = block.T.astype(BF16)
        return total + jnp.sum((block * block).reshape(-1, 8, Z), axis=0)

    def fill(i, carry):
        at = pl.ds(pl.multiple_of(i * TILE, TILE), TILE)
        for j in range(BLK // TILE):
            slot = inv[i * (BLK // TILE) + j]
            tile = values[jnp.maximum(slot, 0)]
            tile = jnp.where(slot >= 0, tile, jnp.zeros_like(tile))
            dense[j // 2, at, (j % 2) * TILE : (j % 2 + 1) * TILE] = tile
        return carry

    with jax.named_scope("sino_in"):
        sino_copy.wait()
    first_ss = looped("read_sino", 0, BLK // 256, read_sino, jnp.zeros((8, Z), F32))
    with jax.named_scope("values_in"):
        values_copy.wait()
    looped("fill", 0, BLK // TILE, fill, 0)

    def row_copy(turn, step, slot):
        return remote(row_ss.at[turn, z], row_ss.at[turn, slot], zs_send, zs_recv, z_id(step))

    def give_norm(turn, total):
        row_ss[turn, z] = total

        def give(step, carry):
            row_copy(turn, step, z).start()
            return carry

        looped("give_norm", 1, NZ, give, 0)

    def take_norm(turn):
        with jax.named_scope("take_norm"):
            took(row_ss.at[turn, pl.ds(0, NZ - 1)], zs_recv)
        return jnp.sqrt(sum_rows(row_ss, turn, NZ) + EPSILON)

    def reduce_copies(turn, message):
        step, unit, units = message
        at = pl.ds(unit, units)
        data = remote(quant.at[turn, at], back.at[turn, at], z_send, z_recv.at[unit], z_id(step))
        scale = remote(quant_scale.at[turn, at], back_scale.at[turn, at], zm_send, zm_recv.at[unit], z_id(step))
        return data, scale

    def send_units(turn, *units):
        for message in REDUCE:
            if message[1] in units:
                for copy in reduce_copies(turn, message):
                    copy.start()

    def await_units(turn, *units):
        for message in REDUCE:
            if message[1] in units:
                for copy in reduce_copies(turn, message):
                    copy.wait_recv()

    def pack(turn, unit, block):
        top = jnp.maximum(jnp.max(jnp.abs(block), axis=0, keepdims=True), 1e-30)
        quant[turn, unit] = jnp.round(block * (32767.0 / top)).astype(jnp.int32).astype(jnp.int16)
        quant_scale[turn, unit] = top * (1.0 / 32767.0)

    def unpack(turn, unit):
        return back[turn, unit].astype(jnp.int32).astype(F32) * back_scale[turn, unit]

    def product(p):
        return jnp.dot(rays_t[...], dense[p], preferred_element_type=F32)

    def backward(turn, norm):
        with jax.named_scope("give_4"):
            block = product(z_at(4))
            pack(turn, 4, block[:, :HV].T)
            pack(turn, 5, block[:, HV:].T)
        if turn == 0:
            with jax.named_scope("barrier"):
                pl.semaphore_wait(barrier, 2 * (NZ - 1) + NQ - 1 + 1)
        send_units(turn, 4, 5)
        give_norm(turn, norm)
        for step, unit in ((3, 0), (-3, 2)):
            with jax.named_scope("give_3"):
                block = product(z_at(step))
                pack(turn, unit, block[:, :HV].T)
                pack(turn, unit + 1, block[:, HV:].T)
                send_units(turn, unit, unit + 1)
        for step, unit in ((1, 6), (-1, 8)):
            with jax.named_scope("give_1"):
                block = product(z_at(step))
                pack(turn, unit, block[:, :HV].T)
                pack(turn, unit + 1, block[:, HV:].T)
                send_units(turn, unit)
        for i, step in enumerate((2, -2)):
            with jax.named_scope("make_2"):
                block = product(z_at(step))
                relay[2 * i] = block[:, :HV].T
                relay[2 * i + 1] = block[:, HV:].T
        with jax.named_scope("make_0"):
            block = product(z)
            own_back[:HV] = block[:, :HV].T
            own_back[HV:] = block[:, HV:].T
        with jax.named_scope("relay_wait"):
            await_units(turn, 0, 4)
        with jax.named_scope("relay"):
            pack(turn, 10, relay[0] + unpack(turn, 0) + unpack(turn, 4))
            send_units(turn, 10)
        with jax.named_scope("relay_wait"):
            await_units(turn, 3, 5)
        with jax.named_scope("relay"):
            pack(turn, 13, relay[3] + unpack(turn, 3) + unpack(turn, 5))
            send_units(turn, 13)
        with jax.named_scope("relay_wait"):
            await_units(turn, 1)
        with jax.named_scope("relay"):
            pack(turn, 11, relay[1] + unpack(turn, 1))
            send_units(turn, 11)
        with jax.named_scope("relay_wait"):
            await_units(turn, 2)
        with jax.named_scope("relay"):
            pack(turn, 12, relay[2] + unpack(turn, 2))
            send_units(turn, 12)
        if turn:
            forward_left(turn - 1)
            took(low.at[turn - 1, pl.ds(0, NZ - 1)], l_recv)
        beta = take_norm(turn)
        with jax.named_scope("reduce_1"):
            await_units(turn, 6, 8)
            own_back[:HV] += unpack(turn, 6) + unpack(turn, 8)
            own_back[HV:] += unpack(turn, 7) + unpack(turn, 9)
        with jax.named_scope("reduce_2"):
            await_units(turn, 10, 13)
            await_units(turn, 11, 12)
        with jax.named_scope("reduce_3"):
            own_back[:HV] += unpack(turn, 10) + unpack(turn, 12)
            own_back[HV:] += unpack(turn, 11) + unpack(turn, 13)
        return beta

    def backward_left(turn):
        left(quant.at[turn], z_send)
        left(quant_scale.at[turn], zm_send)
        left(row_ss.at[turn, pl.ds(0, NZ - 1)], zs_send)
        if turn:
            left(rays.at[turn - 1, core, pl.ds(0, NQ - 1)], g_send)
            left(rays_ss.at[turn - 1, pl.ds(0, NQ - 1)], gs_send)
            left(rays.at[turn - 1, core], r_send)
            left(half_ss.at[turn - 1, 0], n_send)

    def forward_left(turn):
        left(high.at[turn, pl.ds(0, NZ - 1)], h_send)
        left(high_ss.at[turn, pl.ds(0, NZ - 1)], hs_send)
        left(low.at[turn, pl.ds(0, NZ - 1)], l_send)
        left(part_out.at[turn], c_send)
        left(part_ss.at[turn, 0], k_send)
        left(fwd_out.at[turn, pl.ds(0, NQ - 1)], q_send)
        left(fwd_ss.at[turn, pl.ds(0, NQ - 1)], qs_send)

    def gather_copy(turn, k, receiving):
        step, block, half = GATHER[k]
        slot = z_at(block - step if receiving else block)
        rows_at = pl.ds(0, VB) if half is None else pl.ds(half * HV, HV)
        view = high.at[turn, slot, rows_at]
        return remote(view, view, h_send, h_recv.at[k], z_id(step))

    def high_norm(turn, step, slot):
        return remote(high_ss.at[turn, z], high_ss.at[turn, slot], hs_send, hs_recv, z_id(step))

    def low_copy(turn, step, slot):
        return remote(low.at[turn, z], low.at[turn, slot], l_send, l_recv, z_id(step))

    def forward(turn, voxel):
        with jax.named_scope("gather"):
            top = voxel.astype(BF16)
            high[turn, z] = top
            for k in range(6):
                gather_copy(turn, k, False).start()
            low[turn, z] = (voxel - top.astype(F32)).astype(BF16)
            high_ss[turn, z] = squares(voxel)

        def give(step, carry):
            high_norm(turn, step, z).start()
            return carry

        looped("give_norm", 1, NZ, give, 0)
        for arrived, onward in ((0, (6, 8)), (1, (7, 9)), (2, (10,)), (3, (11,))):
            with jax.named_scope("gather_relay"):
                gather_copy(turn, arrived, True).wait_recv()
                for k in onward:
                    gather_copy(turn, k, False).start()
        with jax.named_scope("gather_1"):
            gather_copy(turn, 4, True).wait_recv()
            gather_copy(turn, 5, True).wait_recv()

        def product(at, steps):
            block = None
            for step in steps:
                p = z_at(step)
                term = jnp.dot(dense[p, at, :], high[turn, p], preferred_element_type=F32)
                block = term if block is None else block + term
            return block.reshape(CB, RB, Z)

        near = (0, 1, -1, 2, -2)
        far = (3, -3, 4)

        def theirs_at(i):
            return pl.ds(pl.multiple_of((1 - core) * HALF + i * 256, 256), 256)

        def ours_at(i):
            return pl.ds(pl.multiple_of(core * HALF + i * 256, 256), 256)

        def near_product(i, carry):
            at = pl.ds(i * CB, CB)
            part_out[turn, at] = product(theirs_at(i), near)
            part_own[at] = product(ours_at(i), near)
            return carry

        looped("near_product", 0, HALF // 256, near_product, 0)
        with jax.named_scope("gather_3"):
            for k in (8, 9, 10, 11, 6, 7):
                gather_copy(turn, k, True).wait_recv()

        def give_low(step, carry):
            low_copy(turn, step, z).start()
            return carry

        looped("give_low", 1, NZ, give_low, 0)

        def core_copy(i):
            at = pl.ds(i * CB, CB)
            return remote(part_out.at[turn, at], part_in.at[turn, at], c_send, c_recv, other)

        def theirs(i, carry):
            at = pl.ds(i * CB, CB)
            part_out[turn, at] += product(theirs_at(i), far)
            core_copy(i).start()
            return carry

        looped("theirs", 0, HALF // 256, theirs, 0)

        with jax.named_scope("take_norm"):
            took(high_ss.at[turn, pl.ds(0, NZ - 1)], hs_recv)
        part_ss[turn, 0] = sum_rows(high_ss, turn, NZ)
        core_norm = remote(part_ss.at[turn, 0], part_ss.at[turn, 1], k_send, k_recv, other)
        core_norm.start()

        def ours(i, carry):
            part_own[pl.ds(i * CB, CB)] += product(ours_at(i), far)
            return carry

        looped("ours", 0, HALF // 256, ours, 0)
        with jax.named_scope("core_wait"):
            core_norm.wait_recv()
            chip_ss = part_ss[turn, 0] + part_ss[turn, 1]
            fwd_ss[turn, chip] = chip_ss
            fwd_ss[turn, NQ] = chip_ss
            took(part_in.at[turn], c_recv)
        with jax.named_scope("give_rays"):
            for step in CHIPS:
                q = chip_peer(step)
                fwd_out[turn, q] = (part_own[q] + part_in[turn, q]).astype(BF16)
                remote(fwd_out.at[turn, q], fwd_in.at[turn, chip], q_send, q_recv, chip_id(step)).start()
                remote(fwd_ss.at[turn, NQ], fwd_ss.at[turn, chip], qs_send, qs_recv, chip_id(step)).start()
        backward_left(turn)
        with jax.named_scope("take_rays"):
            took(fwd_ss.at[turn, pl.ds(0, NQ - 1)], qs_recv)
            took(fwd_in.at[turn, pl.ds(0, NQ - 1)], q_recv)
            rays_sum = part_own[chip] + part_in[turn, chip]
            for step in CHIPS:
                rays_sum = rays_sum + fwd_in[turn, chip_from(step)].astype(F32)
        alpha = jnp.sqrt(sum_rows(fwd_ss, turn, NQ) + EPSILON)
        return rays_sum, alpha

    def share_rays(turn, ray, with_data):
        if with_data:
            rays[turn, core, chip] = ray.astype(BF16)
        rays_ss[turn, chip] = squares(ray)

        with jax.named_scope("share"):
            if with_data:
                mine = rays.at[turn, core, chip]
                pass
            for step in CHIPS:
                if with_data:
                    remote(mine, mine, g_send, g_recv, chip_id(step)).start()
                remote(rays_ss.at[turn, chip], rays_ss.at[turn, chip], gs_send, gs_recv, chip_id(step)).start()
        with jax.named_scope("take_share"):
            took(rays_ss.at[turn, pl.ds(0, NQ - 1)], gs_recv)
            if with_data:
                took(rays.at[turn, core, pl.ds(0, NQ - 1)], g_recv)
        half_ss[turn, 0] = sum_rows(rays_ss, turn, NQ)
        if not with_data:
            return half_ss[turn, 0]
        norm = remote(half_ss.at[turn, 0], half_ss.at[turn, 1], n_send, n_recv, other)
        norm.start()
        data = remote(rays.at[turn, core], rays.at[turn, core], r_send, r_recv, other)
        back_data = remote(rays.at[turn, core], rays.at[turn, 1 - core], r_send, r_recv, other)
        data.start()

        def turned(c):
            for i in range(HALF // 256):
                part = rays[turn, c, i * CB : (i + 1) * CB].reshape(256, Z)
                first = pl.multiple_of(c * HALF + i * 256, 256)
                rays_t[:, pl.ds(first, 256)] = part.astype(F32).T.astype(BF16)

        turned(core)
        with jax.named_scope("core_rays"):
            back_data.wait_recv()
        turned(1 - core)
        norm.wait_recv()
        return half_ss[turn, 0] + half_ss[turn, 1]

    beta = backward(0, jnp.sum(first_ss, axis=0, keepdims=True))
    voxel = own_back[...] / beta
    share = sino[pl.ds(pl.multiple_of(core * HALF + chip * RB, RB), RB), :]
    ray_vec = share / beta
    phi_bar = beta
    rho_bar = None
    scale = []
    steps = []
    turns = []
    for turn in range(ITERS):
        rays_sum, alpha = forward(turn, voxel)
        scale.append(alpha)
        if turn == 0:
            rho_bar = alpha
        else:
            theta = sine * alpha
            turns.append(theta / rho)
            rho_bar = -cosine * alpha
        ray_raw = rays_sum / alpha - alpha * ray_vec
        norm = share_rays(turn, ray_raw, turn + 1 < ITERS)
        if turn + 1 < ITERS:
            beta = backward(turn + 1, norm)
            rho = jnp.sqrt(rho_bar * rho_bar + beta * beta)
            cosine = rho_bar / rho
            sine = beta / rho
            phi = cosine * phi_bar
            phi_bar = sine * phi_bar
            steps.append(phi / rho)
            ray_vec = ray_raw / beta
            voxel = own_back[...] / beta - beta * (voxel / alpha)

    weight = [[None] * ITERS for _ in range(ITERS)]
    for k in range(ITERS):
        weight[k][k] = 1.0 / scale[k]
        for j in range(k):
            weight[k][j] = -turns[k - 1] * weight[k - 1][j]
    known = [steps[0] * weight[0][0] + steps[1] * weight[1][0], steps[1] * weight[1][1]]
    final = weight[ITERS - 1]

    place = z * 2 + core
    last_ss[0, place] = norm

    def last_copy(device):
        return remote(last_ss.at[0, place], last_ss.at[0, place], e_send, e_recv, device)

    def give_last(step, carry):
        last_copy(z_id(step)).start()
        last_copy(across_id(step)).start()
        return carry

    looped("give_last", 1, NZ, give_last, 0)
    last_copy(other).start()
    with jax.named_scope("take_low"):
        took(low.at[ITERS - 1, pl.ds(0, NZ - 1)], l_recv)

    def combine(p, carry):
        at = pl.ds(pl.multiple_of(p * VB, VB), VB)
        base = step = None
        for k in range(ITERS):
            value = high[k, p].astype(F32) + low[k, p].astype(F32)
            step = final[k] * value if step is None else step + final[k] * value
            if k < len(known):
                base = known[k] * value if base is None else base + known[k] * value
        done[at, :] = base
        last[at, :] = step
        return carry

    looped("combine", 0, NZ, combine, 0)
    with jax.named_scope("take_last"):
        took(last_ss.at[0, pl.ds(0, 2 * NZ - 1)], e_recv)
    beta = jnp.sqrt(sum_rows(last_ss, 0, 2 * NZ) + EPSILON)
    rho = jnp.sqrt(rho_bar * rho_bar + beta * beta)
    cosine = rho_bar / rho
    sine = beta / rho
    rows[0:1, :] = (cosine * phi_bar) / rho
    rows[1:2, :] = sine * phi_bar

    forward_left(ITERS - 1)
    left(rays_ss.at[ITERS - 1, pl.ds(0, NQ - 1)], gs_send)
    left(last_ss.at[0, pl.ds(0, 2 * NZ - 1)], e_send)


def finish(done, last, rows, out, residual):
    out[...] = done[...] + rows[0:1, :] * last[...]
    residual[...] = rows[1:2, :]


def body(tile_values, tile_rows, tile_cols, tile_count, sinogram):
    values = tile_values[0, 0]
    slots = jnp.arange(tile_rows.shape[-1], dtype=jnp.int32)[None, :]
    targets = jnp.arange((BLK // TILE) ** 2, dtype=jnp.int32)[:, None]
    here = (tile_rows[0] == targets // (BLK // TILE)) & (tile_cols[0] == targets % (BLK // TILE)) & (slots < tile_count)
    inv = jnp.max(jnp.where(here, slots, -1), axis=1)
    dma = pltpu.SemaphoreType.DMA
    vmem = pltpu.VMEM
    tiles = values.shape
    scratch = [
        vmem(tiles, BF16),
        vmem((BLK, Z), F32),
        vmem((NZ, BLK, VB), BF16),
        vmem((Z, BLK), BF16),
        vmem((ITERS, UNITS, HV, Z), jnp.int16),
        vmem((ITERS, UNITS, 1, Z), F32),
        vmem((ITERS, UNITS, HV, Z), jnp.int16),
        vmem((ITERS, UNITS, 1, Z), F32),
        vmem((ITERS, NZ, 1, Z), F32),
        vmem((4, HV, Z), F32),
        vmem((VB, Z), F32),
        vmem((ITERS, NZ, VB, Z), BF16),
        vmem((ITERS, NZ, VB, Z), BF16),
        vmem((ITERS, NZ, 1, Z), F32),
        vmem((NQ, RB, Z), F32),
        vmem((ITERS, NQ, RB, Z), F32),
        vmem((ITERS, NQ, RB, Z), F32),
        vmem((ITERS, 2, 1, Z), F32),
        vmem((ITERS, NQ, RB, Z), BF16),
        vmem((ITERS, NQ, RB, Z), BF16),
        vmem((ITERS, NQ + 1, 1, Z), F32),
        vmem((ITERS - 1, 2, NQ, RB, Z), BF16),
        vmem((ITERS, NQ, 1, Z), F32),
        vmem((ITERS, 2, 1, Z), F32),
        vmem((1, 2 * NZ, 1, Z), F32),
        dma((2,)),
    ]
    for send, recv in (
        ((), (UNITS,)),
        ((), (UNITS,)),
        ((), ()),
        ((), (len(GATHER),)),
        ((), ()),
        ((), ()),
        ((), ()),
        ((), ()),
        ((), ()),
        ((), ()),
        ((), ()),
        ((), ()),
        ((), ()),
        ((), ()),
        ((), ()),
    ):
        scratch += [dma(send), dma(recv)]
    in_vmem = pl.BlockSpec(memory_space=pltpu.VMEM)
    block = jax.ShapeDtypeStruct((BLK, Z), F32)
    done, last, rows = pl.pallas_call(
        kernel,
        out_shape=(block, block, jax.ShapeDtypeStruct((8, Z), F32)),
        in_specs=[
            pl.BlockSpec(memory_space=pltpu.SMEM),
            pl.BlockSpec(memory_space=pltpu.HBM),
            pl.BlockSpec(memory_space=pltpu.HBM),
        ],
        out_specs=(in_vmem, in_vmem, in_vmem),
        scratch_shapes=scratch,
        compiler_params=pltpu.CompilerParams(collective_id=0, has_side_effects=True, vmem_limit_bytes=48 * 1024 * 1024),
    )(inv, values, sinogram)
    found, residual = pl.pallas_call(
        finish,
        out_shape=(block, jax.ShapeDtypeStruct((1, Z), F32)),
        in_specs=[in_vmem, in_vmem, in_vmem],
        out_specs=(in_vmem, in_vmem),
        compiler_params=pltpu.CompilerParams(vmem_limit_bytes=8 * 1024 * 1024),
    )(done, last, rows)
    return found, residual[0]


def solution(mesh):
    split = Mesh(mesh.devices.reshape(NZ, NX, NY, 2), ("row", "cx", "cy", "cc"))
    col = ("cx", "cy", "cc")
    placed = (
        P("row", col, None, None, None),
        P("row", col, None),
        P("row", col, None),
        P("row", col),
        P("row", None),
    )
    return jax.shard_map(body, mesh=split, in_specs=placed, out_specs=(P(col, None), P()), check_vma=False)
```

```python
import jax
import jax.numpy as jnp
from jax import lax
from jax.experimental import pallas as pl
from jax.experimental.pallas import tpu as pltpu
from jax.sharding import Mesh
from jax.sharding import PartitionSpec as P

ITERS = 3
NZ = 8
NX = 4
NY = 4
NQ = NX * NY
TILE = 128
Z = 128
BLK = 2048
VB = BLK // NZ
HV = VB // 2
HALF = BLK // 2
RB = HALF // NQ
CB = 256 // RB
FAR = 512
FB = FAR // RB
EPSILON = 1e-06
MESH = pl.DeviceIdType.MESH
F32 = jnp.float32
BF16 = jnp.bfloat16


def looped(name, first, last, step, carry):
    with jax.named_scope(name):
        return lax.fori_loop(first, last, step, carry)


def squares(x):
    return jnp.sum(x * x, axis=0, keepdims=True)


def sum_rows(ref, turn, count):
    total = ref[turn, 0]
    for i in range(1, count):
        total = total + ref[turn, i]
    return total


GATHER = (
    (2, 0, 0),
    (-2, 0, 1),
    (2, 0, 1),
    (-2, 0, 0),
    (1, 0, None),
    (-1, 0, None),
    (2, -2, 0),
    (-2, 2, 1),
    (1, -2, 0),
    (-1, 2, 1),
    (1, -2, 1),
    (-1, 2, 0),
)
REDUCE = (
    (1, 0, 1),
    (1, 1, 1),
    (-1, 2, 1),
    (-1, 3, 1),
    (2, 4, 1),
    (-2, 5, 1),
    (1, 6, 2),
    (-1, 8, 2),
    (2, 10, 1),
    (2, 11, 1),
    (-2, 12, 1),
    (-2, 13, 1),
)
UNITS = 14
CHIPS = sorted(range(1, NQ), key=lambda step: -(min(step // NY, NX - step // NY) + min(step % NY, NY - step % NY)))


def kernel(
    inv,
    values_hbm,
    sino_hbm,
    done,
    last,
    rows,
    values,
    sino,
    dense,
    rays_t,
    quant,
    quant_scale,
    back,
    back_scale,
    row_ss,
    relay,
    own_back,
    high,
    operand,
    high_ss,
    part_own,
    part_out,
    part_in,
    part_ss,
    fwd_out,
    fwd_in,
    fwd_ss,
    rays,
    rays_ss,
    half_ss,
    last_ss,
    in_sem,
    z_send,
    z_recv,
    zm_send,
    zm_recv,
    zs_send,
    zs_recv,
    h_send,
    h_recv,
    hs_send,
    hs_recv,
    c_send,
    c_recv,
    q_send,
    q_recv,
    qs_send,
    qs_recv,
    g_send,
    g_recv,
    gs_send,
    gs_recv,
    k_send,
    k_recv,
    n_send,
    n_recv,
    r_send,
    r_recv,
    e_send,
    e_recv,
):
    z = lax.axis_index("row")
    cx = lax.axis_index("cx")
    cy = lax.axis_index("cy")
    core = lax.axis_index("cc")
    chip = cx * NY + cy

    def z_at(step):
        return lax.rem(z + (step + NZ), NZ)

    def z_id(step):
        return {"row": z_at(step)}

    def across_id(step):
        return {"row": z_at(step), "cc": 1 - core}

    def chip_at(step):
        return lax.rem(cx + step // NY, NX), lax.rem(cy + lax.rem(step, NY), NY)

    def chip_id(step):
        px, py = chip_at(step)
        return {"cx": px, "cy": py}

    def chip_peer(step):
        px, py = chip_at(step)
        return px * NY + py

    def chip_from(step):
        return lax.rem(cx + NX - step // NY, NX) * NY + lax.rem(cy + NY - lax.rem(step, NY), NY)

    other = {"cc": 1 - core}

    barrier = pltpu.get_barrier_semaphore()

    def greet_z(step, carry):
        pl.semaphore_signal(barrier, inc=1, device_id=z_id(step), device_id_type=MESH)
        return carry

    def greet_chip(step, carry):
        pl.semaphore_signal(barrier, inc=1, device_id=chip_id(step), device_id_type=MESH)
        return carry

    def greet_across(step, carry):
        pl.semaphore_signal(barrier, inc=1, device_id=across_id(step), device_id_type=MESH)
        return carry

    looped("greet_z", 1, NZ, greet_z, 0)
    looped("greet_across", 1, NZ, greet_across, 0)
    looped("greet_chip", 1, NQ, greet_chip, 0)
    pl.semaphore_signal(barrier, inc=1, device_id=other, device_id_type=MESH)

    sino_copy = pltpu.make_async_copy(sino_hbm, sino, in_sem.at[0])
    slots = values_hbm.shape[0]
    values_copy = pltpu.make_async_copy(values_hbm, values.at[pl.ds(0, slots)], in_sem.at[1])
    sino_copy.start()
    values_copy.start()

    def remote(src, dst, send, recv, device):
        return pltpu.make_async_remote_copy(
            src_ref=src, dst_ref=dst, send_sem=send, recv_sem=recv, device_id=device, device_id_type=MESH
        )

    def took(view, sem):
        remote(view, view, sem, sem, other).wait_recv()

    def left(view, sem):
        remote(view, view, sem, sem, other).wait_send()

    def read_sino(i, total):
        at = pl.ds(pl.multiple_of(i * 256, 256), 256)
        block = sino[at, :]
        rays_t[:, at] = block.T.astype(BF16)
        return total + jnp.sum((block * block).reshape(-1, 8, Z), axis=0)

    def fill(i, carry):
        at = pl.ds(pl.multiple_of(i * TILE, TILE), TILE)
        for j in range(BLK // TILE):
            dense[j // 2, at, (j % 2) * TILE : (j % 2 + 1) * TILE] = values[inv[i * (BLK // TILE) + j]]
        return carry

    values[slots] = jnp.zeros((TILE, TILE), BF16)
    with jax.named_scope("sino_in"):
        sino_copy.wait()
    first_ss = looped("read_sino", 0, BLK // 256, read_sino, jnp.zeros((8, Z), F32))
    with jax.named_scope("values_in"):
        values_copy.wait()
    looped("fill", 0, BLK // TILE, fill, 0)

    def row_copy(turn, step, slot):
        return remote(row_ss.at[turn, z], row_ss.at[turn, slot], zs_send, zs_recv, z_id(step))

    def give_norm(turn, total):
        row_ss[turn, z] = total

        def give(step, carry):
            row_copy(turn, step, z).start()
            return carry

        looped("give_norm", 1, NZ, give, 0)

    def take_norm(turn):
        with jax.named_scope("take_norm"):
            took(row_ss.at[turn, pl.ds(0, NZ - 1)], zs_recv)
        return jnp.sqrt(sum_rows(row_ss, turn, NZ) + EPSILON)

    def reduce_copies(turn, message):
        step, unit, units = message
        at = pl.ds(unit, units)
        data = remote(quant.at[turn, at], back.at[turn, at], z_send, z_recv.at[unit], z_id(step))
        scale = remote(quant_scale.at[turn, at], back_scale.at[turn, at], zm_send, zm_recv.at[unit], z_id(step))
        return data, scale

    def send_units(turn, *units):
        for message in REDUCE:
            if message[1] in units:
                for copy in reduce_copies(turn, message):
                    copy.start()

    def await_units(turn, *units):
        for message in REDUCE:
            if message[1] in units:
                for copy in reduce_copies(turn, message):
                    copy.wait_recv()

    def pack(turn, unit, block):
        top = jnp.maximum(jnp.max(jnp.abs(block), axis=0, keepdims=True), 1e-30)
        quant[turn, unit] = jnp.round(block * (32767.0 / top)).astype(jnp.int32).astype(jnp.int16)
        quant_scale[turn, unit] = top * (1.0 / 32767.0)

    def unpack(turn, unit):
        return back[turn, unit].astype(jnp.int32).astype(F32) * back_scale[turn, unit]

    def product(p):
        return jnp.dot(rays_t[...], dense[p], preferred_element_type=F32)

    def backward(turn, norm):
        def halves(step):
            block = product(z_at(step))
            return block[:, :HV], block[:, HV:]

        def pack_both(unit, pair):
            pack(turn, unit, pair[0].T)
            pack(turn, unit + 1, pair[1].T)

        def keep(i, pair):
            relay[2 * i] = pair[0].T
            relay[2 * i + 1] = pair[1].T

        with jax.named_scope("products"):
            first = halves(4)
            second = halves(3)
            pack_both(4, first)
            if turn == 0:
                pl.semaphore_wait(barrier, 2 * (NZ - 1) + NQ - 1 + 1)
            send_units(turn, 4, 5)
            first = halves(-3)
            pack_both(0, second)
            send_units(turn, 0, 1)
            second = halves(1)
            pack_both(2, first)
            send_units(turn, 2, 3)
            if turn:
                meet_norm(turn - 1)
            else:
                give_norm(turn, norm)
            first = halves(-1)
            pack_both(6, second)
            send_units(turn, 6)
            second = halves(2)
            pack_both(8, first)
            send_units(turn, 8)
            first = halves(-2)
            keep(0, second)
            second = halves(0)
            keep(1, first)
            own_back[:HV] = second[0].T
            own_back[HV:] = second[1].T
        if turn:
            give_norm(turn, met_norm(turn - 1))
        with jax.named_scope("relay_wait"):
            await_units(turn, 0, 4)
        with jax.named_scope("relay"):
            pack(turn, 10, relay[0] + unpack(turn, 0) + unpack(turn, 4))
            send_units(turn, 10)
        with jax.named_scope("relay_wait"):
            await_units(turn, 3, 5)
        with jax.named_scope("relay"):
            pack(turn, 13, relay[3] + unpack(turn, 3) + unpack(turn, 5))
            send_units(turn, 13)
        with jax.named_scope("relay_wait"):
            await_units(turn, 1)
        with jax.named_scope("relay"):
            pack(turn, 11, relay[1] + unpack(turn, 1))
            send_units(turn, 11)
        with jax.named_scope("relay_wait"):
            await_units(turn, 2)
        with jax.named_scope("relay"):
            pack(turn, 12, relay[2] + unpack(turn, 2))
            send_units(turn, 12)
        if turn:
            forward_left(turn - 1)
        beta = take_norm(turn)
        with jax.named_scope("reduce_1"):
            await_units(turn, 6, 8)
            own_back[:HV] += unpack(turn, 6) + unpack(turn, 8)
            own_back[HV:] += unpack(turn, 7) + unpack(turn, 9)
        with jax.named_scope("reduce_2"):
            await_units(turn, 10, 13)
            await_units(turn, 11, 12)
        with jax.named_scope("reduce_3"):
            own_back[:HV] += unpack(turn, 10) + unpack(turn, 12)
            own_back[HV:] += unpack(turn, 11) + unpack(turn, 13)
        return beta

    def backward_left(turn):
        left(quant.at[turn], z_send)
        left(quant_scale.at[turn], zm_send)
        left(row_ss.at[turn, pl.ds(0, NZ - 1)], zs_send)
        if turn:
            left(rays.at[turn - 1, core, pl.ds(0, NQ - 1)], g_send)
            left(rays_ss.at[turn - 1, pl.ds(0, NQ - 1)], gs_send)
            left(rays.at[turn - 1, core], r_send)
            left(half_ss.at[turn - 1, 0], n_send)

    def forward_left(turn):
        left(high.at[turn, pl.ds(0, NZ - 1)], h_send)
        left(high_ss.at[turn, pl.ds(0, NZ - 1)], hs_send)
        left(part_out.at[turn], c_send)
        left(part_ss.at[turn, 0], k_send)
        left(fwd_out.at[turn, pl.ds(0, NQ - 1)], q_send)
        left(fwd_ss.at[turn, pl.ds(0, NQ - 1)], qs_send)

    def gather_copy(turn, k, receiving):
        step, block, half = GATHER[k]
        slot = z_at(block - step if receiving else block)
        rows_at = pl.ds(0, VB) if half is None else pl.ds(half * HV, HV)
        view = high.at[turn, slot, rows_at]
        return remote(view, view, h_send, h_recv.at[k], z_id(step))

    def high_norm(turn, step, slot):
        return remote(high_ss.at[turn, z], high_ss.at[turn, slot], hs_send, hs_recv, z_id(step))

    def forward(turn, voxel):
        with jax.named_scope("gather"):
            top = jnp.maximum(jnp.max(jnp.abs(voxel), axis=0, keepdims=True), 1e-30)
            high[turn, z] = jnp.round(voxel * (32767.0 / top)).astype(jnp.int32).astype(jnp.int16)
            high_ss[turn, z, 0] = squares(voxel)
            high_ss[turn, z, 1] = top * (1.0 / 32767.0)
            for step in (4, 3, 5, 2, 6, 1, 7):
                high_norm(turn, step, z).start()
            for k in range(6):
                gather_copy(turn, k, False).start()
            operand[z] = voxel.astype(BF16)
        for arrived, onward in ((0, (6, 8)), (1, (7, 9)), (2, (10,)), (3, (11,))):
            with jax.named_scope("gather_relay"):
                gather_copy(turn, arrived, True).wait_recv()
                for k in onward:
                    gather_copy(turn, k, False).start()
        with jax.named_scope("gather_1"):
            gather_copy(turn, 4, True).wait_recv()
            gather_copy(turn, 5, True).wait_recv()
            took(high_ss.at[turn, pl.ds(0, NZ - 1)], hs_recv)

        def widen(step):
            p = z_at(step)
            operand[p] = (high[turn, p].astype(jnp.int32).astype(F32) * high_ss[turn, p, 1]).astype(BF16)

        with jax.named_scope("widen"):
            for step in (1, -1, 2, -2):
                widen(step)

        def product(at, steps):
            block = None
            for step in steps:
                p = z_at(step)
                term = jnp.dot(dense[p, at, :], operand[p], preferred_element_type=F32)
                block = term if block is None else block + term
            return block.reshape(-1, RB, Z)

        near = (0, 1, -1, 2, -2)
        far = (3, -3, 4)

        def theirs_at(i, count):
            return pl.ds(pl.multiple_of((1 - core) * HALF + i * count, 256), count)

        def ours_at(i, count):
            return pl.ds(pl.multiple_of(core * HALF + i * count, 256), count)

        def near_product(i, carry):
            at = pl.ds(i * CB, CB)
            part_out[turn, at] = product(theirs_at(i, 256), near)
            part_own[at] = product(ours_at(i, 256), near)
            return carry

        looped("near_product", 0, HALF // 256, near_product, 0)
        total = high_ss[turn, 0, 0]
        for i in range(1, NZ):
            total = total + high_ss[turn, i, 0]
        part_ss[turn, 0] = total
        core_norm = remote(part_ss.at[turn, 0], part_ss.at[turn, 1], k_send, k_recv, other)
        core_norm.start()

        with jax.named_scope("gather_3"):
            for k in (8, 9, 10, 11, 6, 7):
                gather_copy(turn, k, True).wait_recv()
        with jax.named_scope("widen"):
            for step in (3, -3, 4):
                widen(step)


        def core_copy(i):
            at = pl.ds(i * FB, FB)
            return remote(part_out.at[turn, at], part_in.at[turn, at], c_send, c_recv, other)

        def theirs(i, carry):
            at = pl.ds(i * FB, FB)
            part_out[turn, at] += product(theirs_at(i, FAR), far)
            core_copy(i).start()
            return carry

        looped("theirs", 0, HALF // FAR, theirs, 0)
        with jax.named_scope("give_alpha"):
            core_norm.wait_recv()
            chip_ss = part_ss[turn, 0] + part_ss[turn, 1]
            fwd_ss[turn, chip] = chip_ss
            fwd_ss[turn, NQ] = chip_ss
            for step in CHIPS:
                remote(fwd_ss.at[turn, NQ], fwd_ss.at[turn, chip], qs_send, qs_recv, chip_id(step)).start()

        def ours(i, carry):
            part_own[pl.ds(i * FB, FB)] += product(ours_at(i, FAR), far)
            return carry

        looped("ours", 0, HALF // FAR, ours, 0)
        with jax.named_scope("core_wait"):
            took(part_in.at[turn], c_recv)
        with jax.named_scope("give_rays"):
            for step in CHIPS:
                q = chip_peer(step)
                fwd_out[turn, q] = (part_own[q] + part_in[turn, q]).astype(BF16)
                remote(fwd_out.at[turn, q], fwd_in.at[turn, chip], q_send, q_recv, chip_id(step)).start()
        backward_left(turn)
        with jax.named_scope("take_rays"):
            took(fwd_ss.at[turn, pl.ds(0, NQ - 1)], qs_recv)
            took(fwd_in.at[turn, pl.ds(0, NQ - 1)], q_recv)
            rays_sum = part_own[chip] + part_in[turn, chip]
            for step in CHIPS:
                rays_sum = rays_sum + fwd_in[turn, chip_from(step)].astype(F32)
        alpha = jnp.sqrt(sum_rows(fwd_ss, turn, NQ) + EPSILON)
        return rays_sum, alpha

    def share_rays(turn, ray, with_data):
        if with_data:
            rays[turn, core, chip] = ray.astype(BF16)
        rays_ss[turn, chip] = squares(ray)

        with jax.named_scope("share"):
            if with_data:
                mine = rays.at[turn, core, chip]
                for step in CHIPS:
                    remote(mine, mine, g_send, g_recv, chip_id(step)).start()
            for step in CHIPS:
                remote(rays_ss.at[turn, chip], rays_ss.at[turn, chip], gs_send, gs_recv, chip_id(step)).start()
        if not with_data:
            with jax.named_scope("take_share"):
                took(rays_ss.at[turn, pl.ds(0, NQ - 1)], gs_recv)
            return sum_rows(rays_ss, turn, NQ)
        with jax.named_scope("take_share"):
            took(rays.at[turn, core, pl.ds(0, NQ - 1)], g_recv)
        data = remote(rays.at[turn, core], rays.at[turn, core], r_send, r_recv, other)
        back_data = remote(rays.at[turn, core], rays.at[turn, 1 - core], r_send, r_recv, other)
        data.start()

        def turned(c):
            for i in range(HALF // 256):
                part = rays[turn, c, i * CB : (i + 1) * CB].reshape(256, Z)
                first = pl.multiple_of(c * HALF + i * 256, 256)
                rays_t[:, pl.ds(first, 256)] = part.astype(F32).T.astype(BF16)

        turned(core)
        with jax.named_scope("core_rays"):
            back_data.wait_recv()
        turned(1 - core)
        return None

    def core_norm_copy(turn):
        return remote(half_ss.at[turn, 0], half_ss.at[turn, 1], n_send, n_recv, other)

    def meet_norm(turn):
        took(rays_ss.at[turn, pl.ds(0, NQ - 1)], gs_recv)
        half_ss[turn, 0] = sum_rows(rays_ss, turn, NQ)
        core_norm_copy(turn).start()

    def met_norm(turn):
        with jax.named_scope("met_norm"):
            core_norm_copy(turn).wait_recv()
        return half_ss[turn, 0] + half_ss[turn, 1]

    beta = backward(0, jnp.sum(first_ss, axis=0, keepdims=True))
    voxel = own_back[...] / beta
    share = sino[pl.ds(pl.multiple_of(core * HALF + chip * RB, RB), RB), :]
    ray_vec = share / beta
    phi_bar = beta
    rho_bar = None
    scale = []
    steps = []
    turns = []
    for turn in range(ITERS):
        rays_sum, alpha = forward(turn, voxel)
        scale.append(alpha)
        if turn == 0:
            rho_bar = alpha
        else:
            theta = sine * alpha
            turns.append(theta / rho)
            rho_bar = -cosine * alpha
        ray_raw = rays_sum / alpha - alpha * ray_vec
        norm = share_rays(turn, ray_raw, turn + 1 < ITERS)
        if turn + 1 < ITERS:
            beta = backward(turn + 1, norm)
            rho = jnp.sqrt(rho_bar * rho_bar + beta * beta)
            cosine = rho_bar / rho
            sine = beta / rho
            phi = cosine * phi_bar
            phi_bar = sine * phi_bar
            steps.append(phi / rho)
            ray_vec = ray_raw / beta
            voxel = own_back[...] / beta - beta * (voxel / alpha)

    weight = [[None] * ITERS for _ in range(ITERS)]
    for k in range(ITERS):
        weight[k][k] = 1.0 / scale[k]
        for j in range(k):
            weight[k][j] = -turns[k - 1] * weight[k - 1][j]
    known = [steps[0] * weight[0][0] + steps[1] * weight[1][0], steps[1] * weight[1][1]]
    final = weight[ITERS - 1]

    place = z * 2 + core
    last_ss[0, place] = norm

    def last_copy(device):
        return remote(last_ss.at[0, place], last_ss.at[0, place], e_send, e_recv, device)

    def give_last(step, carry):
        last_copy(z_id(step)).start()
        last_copy(across_id(step)).start()
        return carry

    looped("give_last", 1, NZ, give_last, 0)
    last_copy(other).start()

    def combine(p, carry):
        at = pl.ds(pl.multiple_of(p * VB, VB), VB)
        base = step = None
        for k in range(ITERS):
            value = high[k, p].astype(jnp.int32).astype(F32) * high_ss[k, p, 1]
            step = final[k] * value if step is None else step + final[k] * value
            if k < len(known):
                base = known[k] * value if base is None else base + known[k] * value
        done[at, :] = base
        last[at, :] = step
        return carry

    looped("combine", 0, NZ, combine, 0)
    with jax.named_scope("take_last"):
        took(last_ss.at[0, pl.ds(0, 2 * NZ - 1)], e_recv)
    beta = jnp.sqrt(sum_rows(last_ss, 0, 2 * NZ) + EPSILON)
    rho = jnp.sqrt(rho_bar * rho_bar + beta * beta)
    cosine = rho_bar / rho
    sine = beta / rho
    rows[0:1, :] = (cosine * phi_bar) / rho
    rows[1:2, :] = sine * phi_bar

    forward_left(ITERS - 1)
    left(rays_ss.at[ITERS - 1, pl.ds(0, NQ - 1)], gs_send)
    left(last_ss.at[0, pl.ds(0, 2 * NZ - 1)], e_send)


def finish(done, last, rows, out, residual):
    out[...] = done[...] + rows[0:1, :] * last[...]
    residual[...] = rows[1:2, :]


def body(tile_values, tile_rows, tile_cols, tile_count, sinogram):
    values = tile_values[0, 0]
    slots = jnp.arange(tile_rows.shape[-1], dtype=jnp.int32)[None, :]
    targets = jnp.arange((BLK // TILE) ** 2, dtype=jnp.int32)[:, None]
    here = (tile_rows[0] == targets // (BLK // TILE)) & (tile_cols[0] == targets % (BLK // TILE)) & (slots < tile_count)
    inv = jnp.min(jnp.where(here, slots, tile_rows.shape[-1]), axis=1)
    dma = pltpu.SemaphoreType.DMA
    vmem = pltpu.VMEM
    tiles = values.shape
    scratch = [
        vmem((tiles[0] + 1, *tiles[1:]), BF16),
        vmem((BLK, Z), F32),
        vmem((NZ, BLK, VB), BF16),
        vmem((Z, BLK), BF16),
        vmem((ITERS, UNITS, HV, Z), jnp.int16),
        vmem((ITERS, UNITS, 1, Z), F32),
        vmem((ITERS, UNITS, HV, Z), jnp.int16),
        vmem((ITERS, UNITS, 1, Z), F32),
        vmem((ITERS, NZ, 1, Z), F32),
        vmem((4, HV, Z), F32),
        vmem((VB, Z), F32),
        vmem((ITERS, NZ, VB, Z), jnp.int16),
        vmem((NZ, VB, Z), BF16),
        vmem((ITERS, NZ, 2, 1, Z), F32),
        vmem((NQ, RB, Z), F32),
        vmem((ITERS, NQ, RB, Z), F32),
        vmem((ITERS, NQ, RB, Z), F32),
        vmem((ITERS, 2, 1, Z), F32),
        vmem((ITERS, NQ, RB, Z), BF16),
        vmem((ITERS, NQ, RB, Z), BF16),
        vmem((ITERS, NQ + 1, 1, Z), F32),
        vmem((ITERS - 1, 2, NQ, RB, Z), BF16),
        vmem((ITERS, NQ, 1, Z), F32),
        vmem((ITERS, 2, 1, Z), F32),
        vmem((1, 2 * NZ, 1, Z), F32),
        dma((2,)),
    ]
    for send, recv in (
        ((), (UNITS,)),
        ((), (UNITS,)),
        ((), ()),
        ((), (len(GATHER),)),
        ((), ()),
        ((), ()),
        ((), ()),
        ((), ()),
        ((), ()),
        ((), ()),
        ((), ()),
        ((), ()),
        ((), ()),
        ((), ()),
    ):
        scratch += [dma(send), dma(recv)]
    in_vmem = pl.BlockSpec(memory_space=pltpu.VMEM)
    block = jax.ShapeDtypeStruct((BLK, Z), F32)
    done, last, rows = pl.pallas_call(
        kernel,
        out_shape=(block, block, jax.ShapeDtypeStruct((8, Z), F32)),
        in_specs=[
            pl.BlockSpec(memory_space=pltpu.SMEM),
            pl.BlockSpec(memory_space=pltpu.HBM),
            pl.BlockSpec(memory_space=pltpu.HBM),
        ],
        out_specs=(in_vmem, in_vmem, in_vmem),
        scratch_shapes=scratch,
        compiler_params=pltpu.CompilerParams(collective_id=0, has_side_effects=True, vmem_limit_bytes=48 * 1024 * 1024),
    )(inv, values, sinogram)
    found, residual = pl.pallas_call(
        finish,
        out_shape=(block, jax.ShapeDtypeStruct((1, Z), F32)),
        in_specs=[in_vmem, in_vmem, in_vmem],
        out_specs=(in_vmem, in_vmem),
        compiler_params=pltpu.CompilerParams(vmem_limit_bytes=8 * 1024 * 1024),
    )(done, last, rows)
    return found, residual[0]


def solution(mesh):
    split = Mesh(mesh.devices.reshape(NZ, NX, NY, 2), ("row", "cx", "cy", "cc"))
    col = ("cx", "cy", "cc")
    placed = (
        P("row", col, None, None, None),
        P("row", col, None),
        P("row", col, None),
        P("row", col),
        P("row", None),
    )
    return jax.shard_map(body, mesh=split, in_specs=placed, out_specs=(P(col, None), P()), check_vma=False)
```

```python
import jax
import jax.numpy as jnp
from jax import lax
from jax.experimental import pallas as pl
from jax.experimental.pallas import tpu as pltpu
from jax.sharding import Mesh
from jax.sharding import PartitionSpec as P

ITERS = 3
NZ = 8
NX = 4
NY = 4
NQ = NX * NY
TILE = 128
Z = 128
BLK = 2048
VB = BLK // NZ
HV = VB // 2
HALF = BLK // 2
RB = HALF // NQ
CB = 256 // RB
FAR = 512
FB = FAR // RB
EPSILON = 1e-06
MESH = pl.DeviceIdType.MESH
F32 = jnp.float32
BF16 = jnp.bfloat16


def looped(name, first, last, step, carry):
    with jax.named_scope(name):
        return lax.fori_loop(first, last, step, carry)


def squares(x):
    return jnp.sum(x * x, axis=0, keepdims=True)


def sum_rows(ref, turn, count):
    total = ref[turn, 0]
    for i in range(1, count):
        total = total + ref[turn, i]
    return total


PIECES = 4
GATHER = [move for i in range(PIECES) for move in ((2, 0, i), (-2, 0, (i + PIECES // 2) % PIECES))] + [(1, 0, None), (-1, 0, None)]
NEAR = len(GATHER)
ONWARD = []
for here in range(2 * PIECES):
    far, _, part = GATHER[here]
    ONWARD.append([])
    for move in ((far, -far, part), (far // 2, -far, part)):
        if move[0] == far and here >= PIECES:
            continue
        ONWARD[here].append(len(GATHER))
        GATHER.append(move)
REDUCE = (
    (1, 0, 1),
    (1, 1, 1),
    (-1, 2, 1),
    (-1, 3, 1),
    (2, 4, 1),
    (-2, 5, 1),
    (1, 6, 2),
    (-1, 8, 2),
    (2, 10, 1),
    (2, 11, 1),
    (-2, 12, 1),
    (-2, 13, 1),
)
UNITS = 14
CHIPS = sorted(range(1, NQ), key=lambda step: -(min(step // NY, NX - step // NY) + min(step % NY, NY - step % NY)))


def kernel(
    inv,
    values_hbm,
    sino_hbm,
    done,
    last,
    rows,
    values,
    sino,
    dense,
    rays_t,
    quant,
    quant_scale,
    back,
    back_scale,
    row_ss,
    relay,
    own_back,
    high,
    operand,
    high_ss,
    part_own,
    part_out,
    part_in,
    part_ss,
    fwd_out,
    fwd_in,
    fwd_ss,
    rays,
    rays_ss,
    half_ss,
    last_ss,
    in_sem,
    z_send,
    z_recv,
    zm_send,
    zm_recv,
    zs_send,
    zs_recv,
    h_send,
    h_recv,
    hs_send,
    hs_recv,
    c_send,
    c_recv,
    q_send,
    q_recv,
    qs_send,
    qs_recv,
    g_send,
    g_recv,
    gs_send,
    gs_recv,
    k_send,
    k_recv,
    n_send,
    n_recv,
    r_send,
    r_recv,
    e_send,
    e_recv,
):
    z = lax.axis_index("row")
    cx = lax.axis_index("cx")
    cy = lax.axis_index("cy")
    core = lax.axis_index("cc")
    chip = cx * NY + cy

    def z_at(step):
        return lax.rem(z + (step + NZ), NZ)

    def z_id(step):
        return {"row": z_at(step)}

    def across_id(step):
        return {"row": z_at(step), "cc": 1 - core}

    def chip_at(step):
        return lax.rem(cx + step // NY, NX), lax.rem(cy + lax.rem(step, NY), NY)

    def chip_id(step):
        px, py = chip_at(step)
        return {"cx": px, "cy": py}

    def chip_peer(step):
        px, py = chip_at(step)
        return px * NY + py

    def chip_from(step):
        return lax.rem(cx + NX - step // NY, NX) * NY + lax.rem(cy + NY - lax.rem(step, NY), NY)

    other = {"cc": 1 - core}

    sino_copy = pltpu.make_async_copy(sino_hbm, sino, in_sem.at[0])
    slots = values_hbm.shape[0]
    values_copy = pltpu.make_async_copy(values_hbm, values.at[pl.ds(0, slots)], in_sem.at[1])
    sino_copy.start()
    values_copy.start()

    barrier = pltpu.get_barrier_semaphore()

    def greet_z(step, carry):
        pl.semaphore_signal(barrier, inc=1, device_id=z_id(step), device_id_type=MESH)
        return carry

    def greet_chip(step, carry):
        pl.semaphore_signal(barrier, inc=1, device_id=chip_id(step), device_id_type=MESH)
        return carry

    def greet_across(step, carry):
        pl.semaphore_signal(barrier, inc=1, device_id=across_id(step), device_id_type=MESH)
        return carry

    looped("greet_z", 1, NZ, greet_z, 0)
    looped("greet_across", 1, NZ, greet_across, 0)
    looped("greet_chip", 1, NQ, greet_chip, 0)
    pl.semaphore_signal(barrier, inc=1, device_id=other, device_id_type=MESH)

    def remote(src, dst, send, recv, device):
        return pltpu.make_async_remote_copy(
            src_ref=src, dst_ref=dst, send_sem=send, recv_sem=recv, device_id=device, device_id_type=MESH
        )

    def took(view, sem):
        remote(view, view, sem, sem, other).wait_recv()

    def left(view, sem):
        remote(view, view, sem, sem, other).wait_send()

    def read_sino(i, total):
        at = pl.ds(pl.multiple_of(i * 256, 256), 256)
        block = sino[at, :]
        rays_t[:, at] = block.T.astype(BF16)
        return total + jnp.sum((block * block).reshape(-1, 8, Z), axis=0)

    def fill(i, carry):
        at = pl.ds(pl.multiple_of(i * TILE, TILE), TILE)
        for j in range(BLK // TILE):
            dense[j // 2, at, (j % 2) * TILE : (j % 2 + 1) * TILE] = values[inv[i * (BLK // TILE) + j]]
        return carry

    values[slots] = jnp.zeros((TILE, TILE), BF16)
    with jax.named_scope("sino_in"):
        sino_copy.wait()
    first_ss = looped("read_sino", 0, BLK // 256, read_sino, jnp.zeros((8, Z), F32))
    with jax.named_scope("values_in"):
        values_copy.wait()
    looped("fill", 0, BLK // TILE, fill, 0)

    def row_copy(turn, step, slot):
        return remote(row_ss.at[turn, z], row_ss.at[turn, slot], zs_send, zs_recv, z_id(step))

    def give_norm(turn, total):
        row_ss[turn, z] = total

        def give(step, carry):
            row_copy(turn, step, z).start()
            return carry

        looped("give_norm", 1, NZ, give, 0)

    def take_norm(turn):
        with jax.named_scope("take_norm"):
            took(row_ss.at[turn, pl.ds(0, NZ - 1)], zs_recv)
        return jnp.sqrt(sum_rows(row_ss, turn, NZ) + EPSILON)

    def reduce_copies(turn, message):
        step, unit, units = message
        at = pl.ds(unit, units)
        data = remote(quant.at[turn, at], back.at[turn, at], z_send, z_recv.at[unit], z_id(step))
        scale = remote(quant_scale.at[turn, at], back_scale.at[turn, at], zm_send, zm_recv.at[unit], z_id(step))
        return data, scale

    def send_units(turn, *units):
        for message in REDUCE:
            if message[1] in units:
                for copy in reduce_copies(turn, message):
                    copy.start()

    def await_units(turn, *units):
        for message in REDUCE:
            if message[1] in units:
                for copy in reduce_copies(turn, message):
                    copy.wait_recv()

    def pack(turn, unit, block):
        top = jnp.maximum(jnp.max(jnp.abs(block), axis=0, keepdims=True), 1e-30)
        quant[turn, unit] = jnp.round(block * (32767.0 / top)).astype(jnp.int32).astype(jnp.int16)
        quant_scale[turn, unit] = top * (1.0 / 32767.0)

    def unpack(turn, unit):
        return back[turn, unit].astype(jnp.int32).astype(F32) * back_scale[turn, unit]

    def product(p):
        return jnp.dot(rays_t[...], dense[p], preferred_element_type=F32)

    def backward(turn, norm):
        def halves(step):
            block = product(z_at(step))
            return block[:, :HV], block[:, HV:]

        def pack_both(unit, pair):
            pack(turn, unit, pair[0].T)
            pack(turn, unit + 1, pair[1].T)

        def keep(i, pair):
            relay[2 * i] = pair[0].T
            relay[2 * i + 1] = pair[1].T

        with jax.named_scope("products"):
            first = halves(4)
            second = halves(3)
            pack_both(4, first)
            if turn == 0:
                pl.semaphore_wait(barrier, 2 * (NZ - 1) + NQ - 1 + 1)
            send_units(turn, 4, 5)
            first = halves(-3)
            pack_both(0, second)
            send_units(turn, 0, 1)
            second = halves(1)
            pack_both(2, first)
            send_units(turn, 2, 3)
            if turn:
                meet_norm(turn - 1)
            else:
                give_norm(turn, norm)
            first = halves(-1)
            pack_both(6, second)
            send_units(turn, 6)
            second = halves(2)
            pack_both(8, first)
            send_units(turn, 8)
            first = halves(-2)
            keep(0, second)
            second = halves(0)
            keep(1, first)
            own_back[:HV] = second[0].T
            own_back[HV:] = second[1].T
        if turn:
            give_norm(turn, met_norm(turn - 1))
        with jax.named_scope("relay_wait"):
            await_units(turn, 0, 4)
        with jax.named_scope("relay"):
            pack(turn, 10, relay[0] + unpack(turn, 0) + unpack(turn, 4))
            send_units(turn, 10)
        with jax.named_scope("relay_wait"):
            await_units(turn, 3, 5)
        with jax.named_scope("relay"):
            pack(turn, 13, relay[3] + unpack(turn, 3) + unpack(turn, 5))
            send_units(turn, 13)
        with jax.named_scope("relay_wait"):
            await_units(turn, 1)
        with jax.named_scope("relay"):
            pack(turn, 11, relay[1] + unpack(turn, 1))
            send_units(turn, 11)
        with jax.named_scope("relay_wait"):
            await_units(turn, 2)
        with jax.named_scope("relay"):
            pack(turn, 12, relay[2] + unpack(turn, 2))
            send_units(turn, 12)
        if turn:
            forward_left(turn - 1)
        beta = take_norm(turn)
        with jax.named_scope("reduce_1"):
            await_units(turn, 6, 8)
            own_back[:HV] += unpack(turn, 6) + unpack(turn, 8)
            own_back[HV:] += unpack(turn, 7) + unpack(turn, 9)
        with jax.named_scope("reduce_2"):
            await_units(turn, 10, 13)
            await_units(turn, 11, 12)
        with jax.named_scope("reduce_3"):
            own_back[:HV] += unpack(turn, 10) + unpack(turn, 12)
            own_back[HV:] += unpack(turn, 11) + unpack(turn, 13)
        return beta

    def backward_left(turn):
        left(quant.at[turn], z_send)
        left(quant_scale.at[turn], zm_send)
        left(row_ss.at[turn, pl.ds(0, NZ - 1)], zs_send)
        if turn:
            left(rays.at[turn - 1, core, pl.ds(0, NQ - 1)], g_send)
            left(rays_ss.at[turn - 1, pl.ds(0, NQ - 1)], gs_send)
            left(rays.at[turn - 1, core], r_send)
            left(half_ss.at[turn - 1, 0], n_send)

    def forward_left(turn):
        left(high.at[turn, pl.ds(0, NZ - 1)], h_send)
        left(high_ss.at[turn, pl.ds(0, NZ - 1)], hs_send)
        left(part_out.at[turn], c_send)
        left(part_ss.at[turn, 0], k_send)
        left(fwd_out.at[turn, pl.ds(0, NQ - 1)], q_send)
        left(fwd_ss.at[turn, pl.ds(0, NQ - 1)], qs_send)

    def gather_copy(turn, k, receiving):
        step, block, part = GATHER[k]
        slot = z_at(block - step if receiving else block)
        rows_at = pl.ds(0, VB) if part is None else pl.ds(part * (VB // PIECES), VB // PIECES)
        view = high.at[turn, slot, rows_at]
        return remote(view, view, h_send, h_recv.at[k], z_id(step))

    def high_norm(turn, step, slot):
        return remote(high_ss.at[turn, z], high_ss.at[turn, slot], hs_send, hs_recv, z_id(step))

    def forward(turn, voxel):
        with jax.named_scope("gather"):
            top = jnp.maximum(jnp.max(jnp.abs(voxel), axis=0, keepdims=True), 1e-30)
            high[turn, z] = jnp.round(voxel * (32767.0 / top)).astype(jnp.int32).astype(jnp.int16)
            high_ss[turn, z, 0] = squares(voxel)
            high_ss[turn, z, 1] = top * (1.0 / 32767.0)
            for step in (4, 3, 5, 2, 6, 1, 7):
                high_norm(turn, step, z).start()
            for k in range(NEAR):
                gather_copy(turn, k, False).start()
            operand[z] = voxel.astype(BF16)
        for arrived, onward in enumerate(ONWARD):
            with jax.named_scope("gather_relay"):
                gather_copy(turn, arrived, True).wait_recv()
                for k in onward:
                    gather_copy(turn, k, False).start()
        with jax.named_scope("gather_1"):
            gather_copy(turn, NEAR - 2, True).wait_recv()
            gather_copy(turn, NEAR - 1, True).wait_recv()
            took(high_ss.at[turn, pl.ds(0, NZ - 1)], hs_recv)

        def widen(step):
            p = z_at(step)
            operand[p] = (high[turn, p].astype(jnp.int32).astype(F32) * high_ss[turn, p, 1]).astype(BF16)

        total = high_ss[turn, 0, 0]
        for i in range(1, NZ):
            total = total + high_ss[turn, i, 0]
        part_ss[turn, 0] = total
        core_norm = remote(part_ss.at[turn, 0], part_ss.at[turn, 1], k_send, k_recv, other)
        core_norm.start()

        with jax.named_scope("widen"):
            for step in (1, -1, 2, -2):
                widen(step)

        def product(at, steps):
            block = None
            for step in steps:
                p = z_at(step)
                term = jnp.dot(dense[p, at, :], operand[p], preferred_element_type=F32)
                block = term if block is None else block + term
            return block.reshape(-1, RB, Z)

        near = (0, 1, -1, 2, -2)
        far = (3, -3, 4)

        def theirs_at(i, count):
            return pl.ds(pl.multiple_of((1 - core) * HALF + i * count, 256), count)

        def ours_at(i, count):
            return pl.ds(pl.multiple_of(core * HALF + i * count, 256), count)

        def near_product(i, carry):
            at = pl.ds(i * CB, CB)
            part_out[turn, at] = product(theirs_at(i, 256), near)
            part_own[at] = product(ours_at(i, 256), near)
            return carry

        looped("near_product", 0, HALF // 256, near_product, 0)
        with jax.named_scope("give_alpha"):
            core_norm.wait_recv()
            chip_ss = part_ss[turn, 0] + part_ss[turn, 1]
            fwd_ss[turn, chip] = chip_ss
            fwd_ss[turn, NQ] = chip_ss
            for step in CHIPS:
                remote(fwd_ss.at[turn, NQ], fwd_ss.at[turn, chip], qs_send, qs_recv, chip_id(step)).start()

        with jax.named_scope("gather_3"):
            for k in range(NEAR, len(GATHER)):
                gather_copy(turn, k, True).wait_recv()
        with jax.named_scope("widen"):
            for step in (3, -3, 4):
                widen(step)


        def core_copy(i):
            at = pl.ds(i * FB, FB)
            return remote(part_out.at[turn, at], part_in.at[turn, at], c_send, c_recv, other)

        def theirs(i, carry):
            at = pl.ds(i * FB, FB)
            part_out[turn, at] += product(theirs_at(i, FAR), far)
            core_copy(i).start()
            return carry

        looped("theirs", 0, HALF // FAR, theirs, 0)
        def ours(i, carry):
            part_own[pl.ds(i * FB, FB)] += product(ours_at(i, FAR), far)
            return carry

        looped("ours", 0, HALF // FAR, ours, 0)
        with jax.named_scope("core_wait"):
            took(part_in.at[turn], c_recv)
        with jax.named_scope("give_rays"):
            for step in CHIPS:
                q = chip_peer(step)
                fwd_out[turn, q] = (part_own[q] + part_in[turn, q]).astype(BF16)
                remote(fwd_out.at[turn, q], fwd_in.at[turn, chip], q_send, q_recv, chip_id(step)).start()
        backward_left(turn)
        with jax.named_scope("take_rays"):
            took(fwd_ss.at[turn, pl.ds(0, NQ - 1)], qs_recv)
            took(fwd_in.at[turn, pl.ds(0, NQ - 1)], q_recv)
            rays_sum = part_own[chip] + part_in[turn, chip]
            for step in CHIPS:
                rays_sum = rays_sum + fwd_in[turn, chip_from(step)].astype(F32)
        alpha = jnp.sqrt(sum_rows(fwd_ss, turn, NQ) + EPSILON)
        return rays_sum, alpha

    def share_rays(turn, ray, with_data):
        if with_data:
            rays[turn, core, chip] = ray.astype(BF16)
        rays_ss[turn, chip] = squares(ray)

        with jax.named_scope("share"):
            if with_data:
                mine = rays.at[turn, core, chip]
                for step in CHIPS:
                    remote(mine, mine, g_send, g_recv, chip_id(step)).start()
            for step in CHIPS:
                remote(rays_ss.at[turn, chip], rays_ss.at[turn, chip], gs_send, gs_recv, chip_id(step)).start()
        if not with_data:
            with jax.named_scope("take_share"):
                took(rays_ss.at[turn, pl.ds(0, NQ - 1)], gs_recv)
            return sum_rows(rays_ss, turn, NQ)
        with jax.named_scope("take_share"):
            took(rays.at[turn, core, pl.ds(0, NQ - 1)], g_recv)
        data = remote(rays.at[turn, core], rays.at[turn, core], r_send, r_recv, other)
        back_data = remote(rays.at[turn, core], rays.at[turn, 1 - core], r_send, r_recv, other)
        data.start()

        def turned(c):
            for i in range(HALF // 256):
                part = rays[turn, c, i * CB : (i + 1) * CB].reshape(256, Z)
                first = pl.multiple_of(c * HALF + i * 256, 256)
                rays_t[:, pl.ds(first, 256)] = part.astype(F32).T.astype(BF16)

        turned(core)
        with jax.named_scope("core_rays"):
            back_data.wait_recv()
        turned(1 - core)
        return None

    def core_norm_copy(turn):
        return remote(half_ss.at[turn, 0], half_ss.at[turn, 1], n_send, n_recv, other)

    def meet_norm(turn):
        took(rays_ss.at[turn, pl.ds(0, NQ - 1)], gs_recv)
        half_ss[turn, 0] = sum_rows(rays_ss, turn, NQ)
        core_norm_copy(turn).start()

    def met_norm(turn):
        with jax.named_scope("met_norm"):
            core_norm_copy(turn).wait_recv()
        return half_ss[turn, 0] + half_ss[turn, 1]

    beta = backward(0, jnp.sum(first_ss, axis=0, keepdims=True))
    voxel = own_back[...] / beta
    share = sino[pl.ds(pl.multiple_of(core * HALF + chip * RB, RB), RB), :]
    ray_vec = share / beta
    phi_bar = beta
    rho_bar = None
    scale = []
    steps = []
    turns = []
    for turn in range(ITERS):
        rays_sum, alpha = forward(turn, voxel)
        scale.append(alpha)
        if turn == 0:
            rho_bar = alpha
        else:
            theta = sine * alpha
            turns.append(theta / rho)
            rho_bar = -cosine * alpha
        ray_raw = rays_sum / alpha - alpha * ray_vec
        norm = share_rays(turn, ray_raw, turn + 1 < ITERS)
        if turn + 1 < ITERS:
            beta = backward(turn + 1, norm)
            rho = jnp.sqrt(rho_bar * rho_bar + beta * beta)
            cosine = rho_bar / rho
            sine = beta / rho
            phi = cosine * phi_bar
            phi_bar = sine * phi_bar
            steps.append(phi / rho)
            ray_vec = ray_raw / beta
            voxel = own_back[...] / beta - beta * (voxel / alpha)

    weight = [[None] * ITERS for _ in range(ITERS)]
    for k in range(ITERS):
        weight[k][k] = 1.0 / scale[k]
        for j in range(k):
            weight[k][j] = -turns[k - 1] * weight[k - 1][j]
    known = [steps[0] * weight[0][0] + steps[1] * weight[1][0], steps[1] * weight[1][1]]
    final = weight[ITERS - 1]

    place = z * 2 + core
    last_ss[0, place] = norm

    def last_copy(device):
        return remote(last_ss.at[0, place], last_ss.at[0, place], e_send, e_recv, device)

    def give_last(step, carry):
        last_copy(z_id(step)).start()
        last_copy(across_id(step)).start()
        return carry

    looped("give_last", 1, NZ, give_last, 0)
    last_copy(other).start()

    def combine(p, carry):
        at = pl.ds(pl.multiple_of(p * VB, VB), VB)
        base = step = None
        for k in range(ITERS):
            value = high[k, p].astype(jnp.int32).astype(F32) * high_ss[k, p, 1]
            step = final[k] * value if step is None else step + final[k] * value
            if k < len(known):
                base = known[k] * value if base is None else base + known[k] * value
        done[at, :] = base
        last[at, :] = step
        return carry

    looped("combine", 0, NZ, combine, 0)
    with jax.named_scope("take_last"):
        took(last_ss.at[0, pl.ds(0, 2 * NZ - 1)], e_recv)
    beta = jnp.sqrt(sum_rows(last_ss, 0, 2 * NZ) + EPSILON)
    rho = jnp.sqrt(rho_bar * rho_bar + beta * beta)
    cosine = rho_bar / rho
    sine = beta / rho
    rows[0:1, :] = (cosine * phi_bar) / rho
    rows[1:2, :] = sine * phi_bar

    forward_left(ITERS - 1)
    left(rays_ss.at[ITERS - 1, pl.ds(0, NQ - 1)], gs_send)
    left(last_ss.at[0, pl.ds(0, 2 * NZ - 1)], e_send)


def finish(done, last, rows, out, residual):
    out[...] = done[...] + rows[0:1, :] * last[...]
    residual[...] = rows[1:2, :]


def body(tile_values, tile_rows, tile_cols, tile_count, sinogram):
    values = tile_values[0, 0]
    slots = jnp.arange(tile_rows.shape[-1], dtype=jnp.int32)[None, :]
    targets = jnp.arange((BLK // TILE) ** 2, dtype=jnp.int32)[:, None]
    here = (tile_rows[0] == targets // (BLK // TILE)) & (tile_cols[0] == targets % (BLK // TILE)) & (slots < tile_count)
    inv = jnp.min(jnp.where(here, slots, tile_rows.shape[-1]), axis=1)
    dma = pltpu.SemaphoreType.DMA
    vmem = pltpu.VMEM
    tiles = values.shape
    scratch = [
        vmem((tiles[0] + 1, *tiles[1:]), BF16),
        vmem((BLK, Z), F32),
        vmem((NZ, BLK, VB), BF16),
        vmem((Z, BLK), BF16),
        vmem((ITERS, UNITS, HV, Z), jnp.int16),
        vmem((ITERS, UNITS, 1, Z), F32),
        vmem((ITERS, UNITS, HV, Z), jnp.int16),
        vmem((ITERS, UNITS, 1, Z), F32),
        vmem((ITERS, NZ, 1, Z), F32),
        vmem((4, HV, Z), F32),
        vmem((VB, Z), F32),
        vmem((ITERS, NZ, VB, Z), jnp.int16),
        vmem((NZ, VB, Z), BF16),
        vmem((ITERS, NZ, 2, 1, Z), F32),
        vmem((NQ, RB, Z), F32),
        vmem((ITERS, NQ, RB, Z), F32),
        vmem((ITERS, NQ, RB, Z), F32),
        vmem((ITERS, 2, 1, Z), F32),
        vmem((ITERS, NQ, RB, Z), BF16),
        vmem((ITERS, NQ, RB, Z), BF16),
        vmem((ITERS, NQ + 1, 1, Z), F32),
        vmem((ITERS - 1, 2, NQ, RB, Z), BF16),
        vmem((ITERS, NQ, 1, Z), F32),
        vmem((ITERS, 2, 1, Z), F32),
        vmem((1, 2 * NZ, 1, Z), F32),
        dma((2,)),
    ]
    for send, recv in (
        ((), (UNITS,)),
        ((), (UNITS,)),
        ((), ()),
        ((), (len(GATHER),)),
        ((), ()),
        ((), ()),
        ((), ()),
        ((), ()),
        ((), ()),
        ((), ()),
        ((), ()),
        ((), ()),
        ((), ()),
        ((), ()),
    ):
        scratch += [dma(send), dma(recv)]
    in_vmem = pl.BlockSpec(memory_space=pltpu.VMEM)
    sinogram = pltpu.with_memory_space_constraint(sinogram, pltpu.HBM)
    block = jax.ShapeDtypeStruct((BLK, Z), F32)
    done, last, rows = pl.pallas_call(
        kernel,
        out_shape=(block, block, jax.ShapeDtypeStruct((8, Z), F32)),
        in_specs=[
            pl.BlockSpec(memory_space=pltpu.SMEM),
            pl.BlockSpec(memory_space=pltpu.HBM),
            pl.BlockSpec(memory_space=pltpu.HBM),
        ],
        out_specs=(in_vmem, in_vmem, in_vmem),
        scratch_shapes=scratch,
        compiler_params=pltpu.CompilerParams(collective_id=0, has_side_effects=True, vmem_limit_bytes=48 * 1024 * 1024),
    )(inv, values, sinogram)
    found, residual = pl.pallas_call(
        finish,
        out_shape=(block, jax.ShapeDtypeStruct((1, Z), F32)),
        in_specs=[in_vmem, in_vmem, in_vmem],
        out_specs=(in_vmem, in_vmem),
        compiler_params=pltpu.CompilerParams(vmem_limit_bytes=8 * 1024 * 1024),
    )(done, last, rows)
    return found, residual[0]


def solution(mesh):
    split = Mesh(mesh.devices.reshape(NZ, NX, NY, 2), ("row", "cx", "cy", "cc"))
    col = ("cx", "cy", "cc")
    placed = (
        P("row", col, None, None, None),
        P("row", col, None),
        P("row", col, None),
        P("row", col),
        P("row", None),
    )
    return jax.shard_map(body, mesh=split, in_specs=placed, out_specs=(P(col, None), P()), check_vma=False)
```

```python
import functools

import jax
import jax.numpy as jnp
from jax import lax
from jax.experimental import pallas as pl
from jax.experimental.pallas import tpu as pltpu
from jax.sharding import Mesh
from jax.sharding import PartitionSpec as P

ITERS = 3
NZ = 8
NX = 4
NY = 4
NQ = NX * NY
TILE = 128
GRID = 16
Z = 128
BLK = 2048
VB = BLK // NZ
HV = VB // 2
HALF = BLK // 2
RB = HALF // NQ
CB = 256 // RB
FAR = 512
FB = FAR // RB
EPSILON = 1e-06
MESH = pl.DeviceIdType.MESH
F32 = jnp.float32
BF16 = jnp.bfloat16


def looped(name, first, last, step, carry):
    with jax.named_scope(name):
        return lax.fori_loop(first, last, step, carry)


def squares(x):
    return jnp.sum(x * x, axis=0, keepdims=True)


def sum_rows(ref, turn, count):
    total = ref[turn, 0]
    for i in range(1, count):
        total = total + ref[turn, i]
    return total


PIECES = 4
GATHER = [move for i in range(PIECES) for move in ((2, 0, i), (-2, 0, (i + PIECES // 2) % PIECES))] + [(1, 0, None), (-1, 0, None)]
NEAR = len(GATHER)
ONWARD = []
for here in range(2 * PIECES):
    far, _, part = GATHER[here]
    ONWARD.append([])
    for move in ((far, -far, part), (far // 2, -far, part)):
        if move[0] == far and here >= PIECES:
            continue
        ONWARD[here].append(len(GATHER))
        GATHER.append(move)
REDUCE = (
    (1, 0, 1),
    (1, 1, 1),
    (-1, 2, 1),
    (-1, 3, 1),
    (2, 4, 1),
    (-2, 5, 1),
    (1, 6, 2),
    (-1, 8, 2),
    (2, 10, 1),
    (2, 11, 1),
    (-2, 12, 1),
    (-2, 13, 1),
)
UNITS = 14
CHIPS = sorted(range(1, NQ), key=lambda step: -(min(step // NY, NX - step // NY) + min(step % NY, NY - step % NY)))


def kernel(
    count,
    rows_hbm,
    cols_hbm,
    values_hbm,
    sino_hbm,
    done,
    last,
    rows,
    values,
    sino,
    dense,
    rays_t,
    quant,
    quant_scale,
    back,
    back_scale,
    row_ss,
    relay,
    own_back,
    high,
    operand,
    high_ss,
    part_own,
    part_out,
    part_in,
    part_ss,
    fwd_out,
    fwd_in,
    fwd_ss,
    rays,
    rays_ss,
    half_ss,
    last_ss,
    places,
    found,
    inv,
    in_sem,
    z_send,
    z_recv,
    zm_send,
    zm_recv,
    zs_send,
    zs_recv,
    h_send,
    h_recv,
    hs_send,
    hs_recv,
    c_send,
    c_recv,
    q_send,
    q_recv,
    qs_send,
    qs_recv,
    g_send,
    g_recv,
    gs_send,
    gs_recv,
    k_send,
    k_recv,
    n_send,
    n_recv,
    r_send,
    r_recv,
    e_send,
    e_recv,
):
    z = lax.axis_index("row")
    cx = lax.axis_index("cx")
    cy = lax.axis_index("cy")
    core = lax.axis_index("cc")
    chip = cx * NY + cy

    def z_at(step):
        return lax.rem(z + (step + NZ), NZ)

    def z_id(step):
        return {"row": z_at(step)}

    def across_id(step):
        return {"row": z_at(step), "cc": 1 - core}

    def chip_at(step):
        return lax.rem(cx + step // NY, NX), lax.rem(cy + lax.rem(step, NY), NY)

    def chip_id(step):
        px, py = chip_at(step)
        return {"cx": px, "cy": py}

    def chip_peer(step):
        px, py = chip_at(step)
        return px * NY + py

    def chip_from(step):
        return lax.rem(cx + NX - step // NY, NX) * NY + lax.rem(cy + NY - lax.rem(step, NY), NY)

    other = {"cc": 1 - core}

    sino_copy = pltpu.make_async_copy(sino_hbm, sino, in_sem.at[0])
    slots = values_hbm.shape[0]
    values_copy = pltpu.make_async_copy(values_hbm, values.at[pl.ds(0, slots)], in_sem.at[1])
    rows_copy = pltpu.make_async_copy(rows_hbm, places.at[0], in_sem.at[3])
    cols_copy = pltpu.make_async_copy(cols_hbm, places.at[1], in_sem.at[4])
    rows_copy.start()
    cols_copy.start()
    sino_copy.start()
    values_copy.start()

    barrier = pltpu.get_barrier_semaphore()

    def greet_z(step, carry):
        pl.semaphore_signal(barrier, inc=1, device_id=z_id(step), device_id_type=MESH)
        return carry

    def greet_chip(step, carry):
        pl.semaphore_signal(barrier, inc=1, device_id=chip_id(step), device_id_type=MESH)
        return carry

    def greet_across(step, carry):
        pl.semaphore_signal(barrier, inc=1, device_id=across_id(step), device_id_type=MESH)
        return carry

    looped("greet_z", 1, NZ, greet_z, 0)
    looped("greet_across", 1, NZ, greet_across, 0)
    looped("greet_chip", 1, NQ, greet_chip, 0)
    pl.semaphore_signal(barrier, inc=1, device_id=other, device_id_type=MESH)

    def remote(src, dst, send, recv, device):
        return pltpu.make_async_remote_copy(
            src_ref=src, dst_ref=dst, send_sem=send, recv_sem=recv, device_id=device, device_id_type=MESH
        )

    def took(view, sem):
        remote(view, view, sem, sem, other).wait_recv()

    def left(view, sem):
        remote(view, view, sem, sem, other).wait_send()

    def read_sino(i, total):
        at = pl.ds(pl.multiple_of(i * 256, 256), 256)
        block = sino[i]
        rays_t[:, at] = block.T.astype(BF16)
        return total + jnp.sum((block * block).reshape(-1, 8, Z), axis=0)

    def fill(half, i, carry):
        at = pl.ds(pl.multiple_of((half * (GRID // 2) + i) * TILE, TILE), TILE)
        for j in range(GRID):
            dense[j // 2, at, (j % 2) * TILE : (j % 2 + 1) * TILE] = values[jnp.clip(inv[half, i * GRID + j], 0, TILE)]
        return carry

    rows_copy.wait()
    cols_copy.wait()
    place = jnp.broadcast_to(places[0] * GRID + places[1], (TILE, TILE)).T
    slot = lax.broadcasted_iota(jnp.int32, (TILE, TILE), 0)
    target = lax.broadcasted_iota(jnp.int32, (TILE, TILE), 1)
    for half in range(2):
        chosen = jnp.where((place == target + half * TILE) & (slot < count[0, 0]), slot, TILE)
        found[half : half + 1] = jnp.min(chosen, axis=0, keepdims=True)
    inv_copy = pltpu.make_async_copy(found.at[pl.ds(0, 2)], inv, in_sem.at[2])
    inv_copy.start()

    values[slots] = jnp.zeros((TILE, TILE), BF16)
    with jax.named_scope("sino_in"):
        sino_copy.wait()
    first_ss = looped("read_sino", 0, BLK // 256, read_sino, jnp.zeros((8, Z), F32))
    with jax.named_scope("values_in"):
        inv_copy.wait()
        values_copy.wait()
    for half in range(2):
        looped("fill", 0, GRID // 2, functools.partial(fill, half), 0)

    def row_copy(turn, step, slot):
        return remote(row_ss.at[turn, z], row_ss.at[turn, slot], zs_send, zs_recv, z_id(step))

    def give_norm(turn, total):
        row_ss[turn, z] = total

        def give(step, carry):
            row_copy(turn, step, z).start()
            return carry

        looped("give_norm", 1, NZ, give, 0)

    def take_norm(turn):
        with jax.named_scope("take_norm"):
            took(row_ss.at[turn, pl.ds(0, NZ - 1)], zs_recv)
        return jnp.sqrt(sum_rows(row_ss, turn, NZ) + EPSILON)

    def reduce_copies(turn, message):
        step, unit, units = message
        at = pl.ds(unit, units)
        data = remote(quant.at[turn, at], back.at[turn, at], z_send, z_recv.at[unit], z_id(step))
        scale = remote(quant_scale.at[turn, at], back_scale.at[turn, at], zm_send, zm_recv.at[unit], z_id(step))
        return data, scale

    def send_units(turn, *units):
        for message in REDUCE:
            if message[1] in units:
                for copy in reduce_copies(turn, message):
                    copy.start()

    def await_units(turn, *units):
        for message in REDUCE:
            if message[1] in units:
                for copy in reduce_copies(turn, message):
                    copy.wait_recv()

    def pack(turn, unit, block):
        top = jnp.maximum(jnp.max(jnp.abs(block), axis=0, keepdims=True), 1e-30)
        quant[turn, unit] = jnp.round(block * (32767.0 / top)).astype(jnp.int32).astype(jnp.int16)
        quant_scale[turn, unit] = top * (1.0 / 32767.0)

    def unpack(turn, unit):
        return back[turn, unit].astype(jnp.int32).astype(F32) * back_scale[turn, unit]

    def product(p):
        return jnp.dot(rays_t[...], dense[p], preferred_element_type=F32)

    def backward(turn, norm):
        def halves(step):
            block = product(z_at(step))
            return block[:, :HV], block[:, HV:]

        def pack_both(unit, pair):
            pack(turn, unit, pair[0].T)
            pack(turn, unit + 1, pair[1].T)

        def keep(i, pair):
            relay[2 * i] = pair[0].T
            relay[2 * i + 1] = pair[1].T

        with jax.named_scope("products"):
            first = halves(4)
            second = halves(3)
            pack_both(4, first)
            if turn == 0:
                pl.semaphore_wait(barrier, 2 * (NZ - 1) + NQ - 1 + 1)
            send_units(turn, 4, 5)
            first = halves(-3)
            pack_both(0, second)
            send_units(turn, 0, 1)
            second = halves(1)
            pack_both(2, first)
            send_units(turn, 2, 3)
            if turn:
                meet_norm(turn - 1)
            else:
                give_norm(turn, norm)
            first = halves(-1)
            pack_both(6, second)
            send_units(turn, 6)
            second = halves(2)
            pack_both(8, first)
            send_units(turn, 8)
            first = halves(-2)
            keep(0, second)
            second = halves(0)
            keep(1, first)
            own_back[:HV] = second[0].T
            own_back[HV:] = second[1].T
        if turn:
            give_norm(turn, met_norm(turn - 1))
        with jax.named_scope("relay_wait"):
            await_units(turn, 0, 4)
        with jax.named_scope("relay"):
            pack(turn, 10, relay[0] + unpack(turn, 0) + unpack(turn, 4))
            send_units(turn, 10)
        with jax.named_scope("relay_wait"):
            await_units(turn, 3, 5)
        with jax.named_scope("relay"):
            pack(turn, 13, relay[3] + unpack(turn, 3) + unpack(turn, 5))
            send_units(turn, 13)
        with jax.named_scope("relay_wait"):
            await_units(turn, 1)
        with jax.named_scope("relay"):
            pack(turn, 11, relay[1] + unpack(turn, 1))
            send_units(turn, 11)
        with jax.named_scope("relay_wait"):
            await_units(turn, 2)
        with jax.named_scope("relay"):
            pack(turn, 12, relay[2] + unpack(turn, 2))
            send_units(turn, 12)
        if turn:
            forward_left(turn - 1)
        beta = take_norm(turn)
        with jax.named_scope("reduce_1"):
            await_units(turn, 6, 8)
            own_back[:HV] += unpack(turn, 6) + unpack(turn, 8)
            own_back[HV:] += unpack(turn, 7) + unpack(turn, 9)
        with jax.named_scope("reduce_2"):
            await_units(turn, 10, 13)
            await_units(turn, 11, 12)
        with jax.named_scope("reduce_3"):
            own_back[:HV] += unpack(turn, 10) + unpack(turn, 12)
            own_back[HV:] += unpack(turn, 11) + unpack(turn, 13)
        return beta

    def backward_left(turn):
        left(quant.at[turn], z_send)
        left(quant_scale.at[turn], zm_send)
        left(row_ss.at[turn, pl.ds(0, NZ - 1)], zs_send)
        if turn:
            left(rays.at[turn - 1, core, pl.ds(0, NQ - 1)], g_send)
            left(rays_ss.at[turn - 1, pl.ds(0, NQ - 1)], gs_send)
            left(rays.at[turn - 1, core], r_send)
            left(half_ss.at[turn - 1, 0], n_send)

    def forward_left(turn):
        left(high.at[turn, pl.ds(0, NZ - 1)], h_send)
        left(high_ss.at[turn, pl.ds(0, NZ - 1)], hs_send)
        left(part_out.at[turn], c_send)
        left(part_ss.at[turn, 0], k_send)
        left(fwd_out.at[turn, pl.ds(0, NQ - 1)], q_send)
        left(fwd_ss.at[turn, pl.ds(0, NQ - 1)], qs_send)

    def gather_copy(turn, k, receiving):
        step, block, part = GATHER[k]
        slot = z_at(block - step if receiving else block)
        rows_at = pl.ds(0, VB) if part is None else pl.ds(part * (VB // PIECES), VB // PIECES)
        view = high.at[turn, slot, rows_at]
        return remote(view, view, h_send, h_recv.at[k], z_id(step))

    def high_norm(turn, step, slot):
        return remote(high_ss.at[turn, z], high_ss.at[turn, slot], hs_send, hs_recv, z_id(step))

    def forward(turn, voxel):
        with jax.named_scope("gather"):
            top = jnp.maximum(jnp.max(jnp.abs(voxel), axis=0, keepdims=True), 1e-30)
            high[turn, z] = jnp.round(voxel * (32767.0 / top)).astype(jnp.int32).astype(jnp.int16)
            high_ss[turn, z, 0] = squares(voxel)
            high_ss[turn, z, 1] = top * (1.0 / 32767.0)
            for step in (4, 3, 5, 2, 6, 1, 7):
                high_norm(turn, step, z).start()
            for k in range(NEAR):
                gather_copy(turn, k, False).start()
            operand[z] = voxel.astype(BF16)
        for arrived, onward in enumerate(ONWARD):
            with jax.named_scope("gather_relay"):
                gather_copy(turn, arrived, True).wait_recv()
                for k in onward:
                    gather_copy(turn, k, False).start()
        with jax.named_scope("gather_1"):
            gather_copy(turn, NEAR - 2, True).wait_recv()
            gather_copy(turn, NEAR - 1, True).wait_recv()
            took(high_ss.at[turn, pl.ds(0, NZ - 1)], hs_recv)

        def widen(step):
            p = z_at(step)
            operand[p] = (high[turn, p].astype(jnp.int32).astype(F32) * high_ss[turn, p, 1]).astype(BF16)

        total = high_ss[turn, 0, 0]
        for i in range(1, NZ):
            total = total + high_ss[turn, i, 0]
        part_ss[turn, 0] = total
        core_norm = remote(part_ss.at[turn, 0], part_ss.at[turn, 1], k_send, k_recv, other)
        core_norm.start()

        with jax.named_scope("widen"):
            for step in (1, -1, 2, -2):
                widen(step)

        def product(at, steps):
            block = None
            for step in steps:
                p = z_at(step)
                term = jnp.dot(dense[p, at, :], operand[p], preferred_element_type=F32)
                block = term if block is None else block + term
            return block.reshape(-1, RB, Z)

        near = (0, 1, -1, 2, -2)
        far = (3, -3, 4)

        def theirs_at(i, count):
            return pl.ds(pl.multiple_of((1 - core) * HALF + i * count, 256), count)

        def ours_at(i, count):
            return pl.ds(pl.multiple_of(core * HALF + i * count, 256), count)

        def near_product(i, carry):
            at = pl.ds(i * CB, CB)
            part_out[turn, at] = product(theirs_at(i, 256), near)
            part_own[at] = product(ours_at(i, 256), near)
            return carry

        looped("near_product", 0, HALF // 256, near_product, 0)
        with jax.named_scope("give_alpha"):
            core_norm.wait_recv()
            chip_ss = part_ss[turn, 0] + part_ss[turn, 1]
            fwd_ss[turn, chip] = chip_ss
            fwd_ss[turn, NQ] = chip_ss
            for step in CHIPS:
                remote(fwd_ss.at[turn, NQ], fwd_ss.at[turn, chip], qs_send, qs_recv, chip_id(step)).start()

        with jax.named_scope("gather_3"):
            for k in range(NEAR, len(GATHER)):
                gather_copy(turn, k, True).wait_recv()
        with jax.named_scope("widen"):
            for step in (3, -3, 4):
                widen(step)


        def core_copy(i):
            at = pl.ds(i * FB, FB)
            return remote(part_out.at[turn, at], part_in.at[turn, at], c_send, c_recv, other)

        def theirs(i, carry):
            at = pl.ds(i * FB, FB)
            part_out[turn, at] += product(theirs_at(i, FAR), far)
            core_copy(i).start()
            return carry

        looped("theirs", 0, HALF // FAR, theirs, 0)
        def ours(i, carry):
            part_own[pl.ds(i * FB, FB)] += product(ours_at(i, FAR), far)
            return carry

        looped("ours", 0, HALF // FAR, ours, 0)
        with jax.named_scope("core_wait"):
            took(part_in.at[turn], c_recv)
        with jax.named_scope("give_rays"):
            for step in CHIPS:
                q = chip_peer(step)
                fwd_out[turn, q] = (part_own[q] + part_in[turn, q]).astype(BF16)
                remote(fwd_out.at[turn, q], fwd_in.at[turn, chip], q_send, q_recv, chip_id(step)).start()
        backward_left(turn)
        with jax.named_scope("take_rays"):
            took(fwd_ss.at[turn, pl.ds(0, NQ - 1)], qs_recv)
            took(fwd_in.at[turn, pl.ds(0, NQ - 1)], q_recv)
            rays_sum = part_own[chip] + part_in[turn, chip]
            for step in CHIPS:
                rays_sum = rays_sum + fwd_in[turn, chip_from(step)].astype(F32)
        alpha = jnp.sqrt(sum_rows(fwd_ss, turn, NQ) + EPSILON)
        return rays_sum, alpha

    def share_rays(turn, ray, with_data):
        if with_data:
            rays[turn, core, chip] = ray.astype(BF16)
        rays_ss[turn, chip] = squares(ray)

        with jax.named_scope("share"):
            if with_data:
                mine = rays.at[turn, core, chip]
                for step in CHIPS:
                    remote(mine, mine, g_send, g_recv, chip_id(step)).start()
            for step in CHIPS:
                remote(rays_ss.at[turn, chip], rays_ss.at[turn, chip], gs_send, gs_recv, chip_id(step)).start()
        if not with_data:
            with jax.named_scope("take_share"):
                took(rays_ss.at[turn, pl.ds(0, NQ - 1)], gs_recv)
            return sum_rows(rays_ss, turn, NQ)
        with jax.named_scope("take_share"):
            took(rays.at[turn, core, pl.ds(0, NQ - 1)], g_recv)
        data = remote(rays.at[turn, core], rays.at[turn, core], r_send, r_recv, other)
        back_data = remote(rays.at[turn, core], rays.at[turn, 1 - core], r_send, r_recv, other)
        data.start()

        def turned(c):
            for i in range(HALF // 256):
                part = rays[turn, c, i * CB : (i + 1) * CB].reshape(256, Z)
                first = pl.multiple_of(c * HALF + i * 256, 256)
                rays_t[:, pl.ds(first, 256)] = part.astype(F32).T.astype(BF16)

        turned(core)
        with jax.named_scope("core_rays"):
            back_data.wait_recv()
        turned(1 - core)
        return None

    def core_norm_copy(turn):
        return remote(half_ss.at[turn, 0], half_ss.at[turn, 1], n_send, n_recv, other)

    def meet_norm(turn):
        took(rays_ss.at[turn, pl.ds(0, NQ - 1)], gs_recv)
        half_ss[turn, 0] = sum_rows(rays_ss, turn, NQ)
        core_norm_copy(turn).start()

    def met_norm(turn):
        with jax.named_scope("met_norm"):
            core_norm_copy(turn).wait_recv()
        return half_ss[turn, 0] + half_ss[turn, 1]

    beta = backward(0, jnp.sum(first_ss, axis=0, keepdims=True))
    voxel = own_back[...] / beta
    share = sino[core * (HALF // 256) + chip // CB, pl.ds(pl.multiple_of(lax.rem(chip, CB) * RB, RB), RB), :]
    ray_vec = share / beta
    phi_bar = beta
    rho_bar = None
    scale = []
    steps = []
    turns = []
    for turn in range(ITERS):
        rays_sum, alpha = forward(turn, voxel)
        scale.append(alpha)
        if turn == 0:
            rho_bar = alpha
        else:
            theta = sine * alpha
            turns.append(theta / rho)
            rho_bar = -cosine * alpha
        ray_raw = rays_sum / alpha - alpha * ray_vec
        norm = share_rays(turn, ray_raw, turn + 1 < ITERS)
        if turn + 1 < ITERS:
            beta = backward(turn + 1, norm)
            rho = jnp.sqrt(rho_bar * rho_bar + beta * beta)
            cosine = rho_bar / rho
            sine = beta / rho
            phi = cosine * phi_bar
            phi_bar = sine * phi_bar
            steps.append(phi / rho)
            ray_vec = ray_raw / beta
            voxel = own_back[...] / beta - beta * (voxel / alpha)

    weight = [[None] * ITERS for _ in range(ITERS)]
    for k in range(ITERS):
        weight[k][k] = 1.0 / scale[k]
        for j in range(k):
            weight[k][j] = -turns[k - 1] * weight[k - 1][j]
    known = [steps[0] * weight[0][0] + steps[1] * weight[1][0], steps[1] * weight[1][1]]
    final = weight[ITERS - 1]

    place = z * 2 + core
    last_ss[0, place] = norm

    def last_copy(device):
        return remote(last_ss.at[0, place], last_ss.at[0, place], e_send, e_recv, device)

    def give_last(step, carry):
        last_copy(z_id(step)).start()
        last_copy(across_id(step)).start()
        return carry

    looped("give_last", 1, NZ, give_last, 0)
    last_copy(other).start()

    def combine(p, carry):
        at = pl.ds(pl.multiple_of(p * VB, VB), VB)
        base = step = None
        for k in range(ITERS):
            value = high[k, p].astype(jnp.int32).astype(F32) * high_ss[k, p, 1]
            step = final[k] * value if step is None else step + final[k] * value
            if k < len(known):
                base = known[k] * value if base is None else base + known[k] * value
        done[at, :] = base
        last[at, :] = step
        return carry

    looped("combine", 0, NZ, combine, 0)
    with jax.named_scope("take_last"):
        took(last_ss.at[0, pl.ds(0, 2 * NZ - 1)], e_recv)
    beta = jnp.sqrt(sum_rows(last_ss, 0, 2 * NZ) + EPSILON)
    rho = jnp.sqrt(rho_bar * rho_bar + beta * beta)
    cosine = rho_bar / rho
    sine = beta / rho
    rows[0:1, :] = (cosine * phi_bar) / rho
    rows[1:2, :] = sine * phi_bar

    forward_left(ITERS - 1)
    left(rays_ss.at[ITERS - 1, pl.ds(0, NQ - 1)], gs_send)
    left(last_ss.at[0, pl.ds(0, 2 * NZ - 1)], e_send)


def finish(done, last, rows, out, residual):
    out[...] = done[...] + rows[0:1, :] * last[...]
    residual[...] = rows[1:2, :]


def stay(array):
    return pltpu.with_memory_space_constraint(array, pltpu.HBM)


def body(tile_values, tile_rows, tile_cols, tile_count, sinogram):
    values = tile_values[0, 0]
    dma = pltpu.SemaphoreType.DMA
    vmem = pltpu.VMEM
    tiles = values.shape
    scratch = [
        vmem((tiles[0] + 1, *tiles[1:]), BF16),
        vmem((BLK // 256, 256, Z), F32),
        vmem((NZ, BLK, VB), BF16),
        vmem((Z, BLK), BF16),
        vmem((ITERS, UNITS, HV, Z), jnp.int16),
        vmem((ITERS, UNITS, 1, Z), F32),
        vmem((ITERS, UNITS, HV, Z), jnp.int16),
        vmem((ITERS, UNITS, 1, Z), F32),
        vmem((ITERS, NZ, 1, Z), F32),
        vmem((4, HV, Z), F32),
        vmem((VB, Z), F32),
        vmem((ITERS, NZ, VB, Z), jnp.int16),
        vmem((NZ, VB, Z), BF16),
        vmem((ITERS, NZ, 2, 1, Z), F32),
        vmem((NQ, RB, Z), F32),
        vmem((ITERS, NQ, RB, Z), F32),
        vmem((ITERS, NQ, RB, Z), F32),
        vmem((ITERS, 2, 1, Z), F32),
        vmem((ITERS, NQ, RB, Z), BF16),
        vmem((ITERS, NQ, RB, Z), BF16),
        vmem((ITERS, NQ + 1, 1, Z), F32),
        vmem((ITERS - 1, 2, NQ, RB, Z), BF16),
        vmem((ITERS, NQ, 1, Z), F32),
        vmem((ITERS, 2, 1, Z), F32),
        vmem((1, 2 * NZ, 1, Z), F32),
        vmem((2, 1, TILE), jnp.int32),
        vmem((8, TILE), jnp.int32),
        pltpu.SMEM((2, TILE), jnp.int32),
        dma((5,)),
    ]
    for send, recv in (
        ((), (UNITS,)),
        ((), (UNITS,)),
        ((), ()),
        ((), (len(GATHER),)),
        ((), ()),
        ((), ()),
        ((), ()),
        ((), ()),
        ((), ()),
        ((), ()),
        ((), ()),
        ((), ()),
        ((), ()),
        ((), ()),
    ):
        scratch += [dma(send), dma(recv)]
    in_vmem = pl.BlockSpec(memory_space=pltpu.VMEM)
    block = jax.ShapeDtypeStruct((BLK, Z), F32)
    done, last, rows = pl.pallas_call(
        kernel,
        out_shape=(block, block, jax.ShapeDtypeStruct((8, Z), F32)),
        in_specs=[
            pl.BlockSpec(memory_space=pltpu.SMEM),
            pl.BlockSpec(memory_space=pltpu.HBM),
            pl.BlockSpec(memory_space=pltpu.HBM),
            pl.BlockSpec(memory_space=pltpu.HBM),
            pl.BlockSpec(memory_space=pltpu.HBM),
        ],
        out_specs=(in_vmem, in_vmem, in_vmem),
        scratch_shapes=scratch,
        compiler_params=pltpu.CompilerParams(collective_id=0, has_side_effects=True, vmem_limit_bytes=48 * 1024 * 1024),
    )(tile_count, stay(tile_rows[0]), stay(tile_cols[0]), values, stay(sinogram.reshape(BLK // 256, 256, Z)))
    found, residual = pl.pallas_call(
        finish,
        out_shape=(block, jax.ShapeDtypeStruct((1, Z), F32)),
        in_specs=[in_vmem, in_vmem, in_vmem],
        out_specs=(in_vmem, in_vmem),
        compiler_params=pltpu.CompilerParams(vmem_limit_bytes=8 * 1024 * 1024),
    )(done, last, rows)
    return found, residual[0]


def solution(mesh):
    split = Mesh(mesh.devices.reshape(NZ, NX, NY, 2), ("row", "cx", "cy", "cc"))
    col = ("cx", "cy", "cc")
    placed = (
        P("row", col, None, None, None),
        P("row", col, None),
        P("row", col, None),
        P("row", col),
        P("row", None),
    )
    return jax.shard_map(body, mesh=split, in_specs=placed, out_specs=(P(col, None), P()), check_vma=False)
```

```python
import functools

import jax
import jax.numpy as jnp
from jax import lax
from jax.experimental import pallas as pl
from jax.experimental.pallas import tpu as pltpu
from jax.sharding import Mesh
from jax.sharding import PartitionSpec as P

ITERS = 3
NZ = 8
NX = 4
NY = 4
NQ = NX * NY
TILE = 128
GRID = 16
Z = 128
BLK = 2048
VB = BLK // NZ
HV = VB // 2
HALF = BLK // 2
RB = HALF // NQ
CB = 256 // RB
FAR = 512
FB = FAR // RB
EPSILON = 1e-06
MESH = pl.DeviceIdType.MESH
F32 = jnp.float32
BF16 = jnp.bfloat16


def looped(name, first, last, step, carry):
    with jax.named_scope(name):
        return lax.fori_loop(first, last, step, carry)


def squares(x):
    return jnp.sum(x * x, axis=0, keepdims=True)


def sum_rows(ref, turn, count):
    total = ref[turn, 0]
    for i in range(1, count):
        total = total + ref[turn, i]
    return total


PIECES = 4
GATHER = [move for i in range(PIECES) for move in ((2, 0, i), (-2, 0, (i + PIECES // 2) % PIECES))] + [(1, 0, None), (-1, 0, None)]
NEAR = len(GATHER)
ONWARD = []
for here in range(2 * PIECES):
    far, _, part = GATHER[here]
    ONWARD.append([])
    for move in ((far, -far, part), (far // 2, -far, part)):
        if move[0] == far and here >= PIECES:
            continue
        ONWARD[here].append(len(GATHER))
        GATHER.append(move)
REDUCE = (
    (1, 0, 1),
    (1, 1, 1),
    (-1, 2, 1),
    (-1, 3, 1),
    (2, 4, 1),
    (-2, 5, 1),
    (1, 6, 2),
    (-1, 8, 2),
    (2, 10, 1),
    (2, 11, 1),
    (-2, 12, 1),
    (-2, 13, 1),
)
UNITS = 14
CHIPS = sorted(range(1, NQ), key=lambda step: -(min(step // NY, NX - step // NY) + min(step % NY, NY - step % NY)))


def kernel(
    count,
    rows_hbm,
    cols_hbm,
    values_hbm,
    sino_hbm,
    done,
    last,
    rows,
    values,
    sino,
    dense,
    rays_t,
    quant,
    quant_scale,
    back,
    back_scale,
    row_ss,
    relay,
    own_back,
    high,
    operand,
    high_ss,
    part_own,
    part_out,
    part_in,
    part_ss,
    fwd_out,
    fwd_in,
    fwd_ss,
    rays,
    rays_ss,
    half_ss,
    last_ss,
    places,
    found,
    inv,
    in_sem,
    z_send,
    z_recv,
    zm_send,
    zm_recv,
    zs_send,
    zs_recv,
    h_send,
    h_recv,
    hs_send,
    hs_recv,
    c_send,
    c_recv,
    q_send,
    q_recv,
    qs_send,
    qs_recv,
    g_send,
    g_recv,
    gs_send,
    gs_recv,
    k_send,
    k_recv,
    n_send,
    n_recv,
    r_send,
    r_recv,
    e_send,
    e_recv,
):
    z = lax.axis_index("row")
    cx = lax.axis_index("cx")
    cy = lax.axis_index("cy")
    core = lax.axis_index("cc")
    chip = cx * NY + cy

    def z_at(step):
        return lax.rem(z + (step + NZ), NZ)

    def z_id(step):
        return {"row": z_at(step)}

    def across_id(step):
        return {"row": z_at(step), "cc": 1 - core}

    def chip_at(step):
        return lax.rem(cx + step // NY, NX), lax.rem(cy + lax.rem(step, NY), NY)

    def chip_id(step):
        px, py = chip_at(step)
        return {"cx": px, "cy": py}

    def chip_peer(step):
        px, py = chip_at(step)
        return px * NY + py

    def chip_from(step):
        return lax.rem(cx + NX - step // NY, NX) * NY + lax.rem(cy + NY - lax.rem(step, NY), NY)

    other = {"cc": 1 - core}

    sino_copy = pltpu.make_async_copy(sino_hbm, sino, in_sem.at[0])
    slots = values_hbm.shape[0]
    values_copy = pltpu.make_async_copy(values_hbm, values.at[pl.ds(0, slots)], in_sem.at[1])
    rows_copy = pltpu.make_async_copy(rows_hbm, places.at[0], in_sem.at[3])
    cols_copy = pltpu.make_async_copy(cols_hbm, places.at[1], in_sem.at[4])
    rows_copy.start()
    cols_copy.start()
    sino_copy.start()
    values_copy.start()

    barrier = pltpu.get_barrier_semaphore()

    def greet_z(step, carry):
        pl.semaphore_signal(barrier, inc=1, device_id=z_id(step), device_id_type=MESH)
        return carry

    def greet_chip(step, carry):
        pl.semaphore_signal(barrier, inc=1, device_id=chip_id(step), device_id_type=MESH)
        return carry

    def greet_across(step, carry):
        pl.semaphore_signal(barrier, inc=1, device_id=across_id(step), device_id_type=MESH)
        return carry

    looped("greet_z", 1, NZ, greet_z, 0)
    looped("greet_across", 1, NZ, greet_across, 0)
    looped("greet_chip", 1, NQ, greet_chip, 0)
    pl.semaphore_signal(barrier, inc=1, device_id=other, device_id_type=MESH)

    def remote(src, dst, send, recv, device):
        return pltpu.make_async_remote_copy(
            src_ref=src, dst_ref=dst, send_sem=send, recv_sem=recv, device_id=device, device_id_type=MESH
        )

    def took(view, sem):
        remote(view, view, sem, sem, other).wait_recv()

    def left(view, sem):
        remote(view, view, sem, sem, other).wait_send()

    def read_sino(i, total):
        at = pl.ds(pl.multiple_of(i * 256, 256), 256)
        block = sino[i]
        rays_t[:, at] = block.T.astype(BF16)
        return total + jnp.sum((block * block).reshape(-1, 8, Z), axis=0)

    def fill(half, i, carry):
        at = pl.ds(pl.multiple_of((half * (GRID // 2) + i) * TILE, TILE), TILE)
        for j in range(GRID):
            dense[j // 2, at, (j % 2) * TILE : (j % 2 + 1) * TILE] = values[inv[half, i * GRID + j]]
        return carry

    rows_copy.wait()
    cols_copy.wait()
    place = jnp.broadcast_to(places[0] * GRID + places[1], (TILE, TILE)).T
    slot = lax.broadcasted_iota(jnp.int32, (TILE, TILE), 0)
    target = lax.broadcasted_iota(jnp.int32, (TILE, TILE), 1)
    for half in range(2):
        chosen = jnp.where((place == target + half * TILE) & (slot < count[0, 0]), slot, TILE)
        found[half : half + 1] = jnp.min(chosen, axis=0, keepdims=True)
    inv_copy = pltpu.make_async_copy(found.at[pl.ds(0, 2)], inv, in_sem.at[2])
    inv_copy.start()

    values[slots] = jnp.zeros((TILE, TILE), BF16)
    with jax.named_scope("sino_in"):
        sino_copy.wait()
    first_ss = looped("read_sino", 0, BLK // 256, read_sino, jnp.zeros((8, Z), F32))
    with jax.named_scope("values_in"):
        inv_copy.wait()
        values_copy.wait()
    for half in range(2):
        looped("fill", 0, GRID // 2, functools.partial(fill, half), 0)

    def row_copy(turn, step, slot):
        return remote(row_ss.at[turn, z], row_ss.at[turn, slot], zs_send, zs_recv, z_id(step))

    def give_norm(turn, total):
        row_ss[turn, z] = total

        def give(step, carry):
            row_copy(turn, step, z).start()
            return carry

        looped("give_norm", 1, NZ, give, 0)

    def take_norm(turn):
        with jax.named_scope("take_norm"):
            took(row_ss.at[turn, pl.ds(0, NZ - 1)], zs_recv)
        return jnp.sqrt(sum_rows(row_ss, turn, NZ) + EPSILON)

    def reduce_copies(turn, message):
        step, unit, units = message
        at = pl.ds(unit, units)
        data = remote(quant.at[turn, at], back.at[turn, at], z_send, z_recv.at[unit], z_id(step))
        scale = remote(quant_scale.at[turn, at], back_scale.at[turn, at], zm_send, zm_recv.at[unit], z_id(step))
        return data, scale

    def send_units(turn, *units):
        for message in REDUCE:
            if message[1] in units:
                for copy in reduce_copies(turn, message):
                    copy.start()

    def await_units(turn, *units):
        for message in REDUCE:
            if message[1] in units:
                for copy in reduce_copies(turn, message):
                    copy.wait_recv()

    def pack(turn, unit, block):
        top = jnp.maximum(jnp.max(jnp.abs(block), axis=0, keepdims=True), 1e-30)
        quant[turn, unit] = jnp.round(block * (32767.0 / top)).astype(jnp.int32).astype(jnp.int16)
        quant_scale[turn, unit] = top * (1.0 / 32767.0)

    def unpack(turn, unit):
        return back[turn, unit].astype(jnp.int32).astype(F32) * back_scale[turn, unit]

    def product(p):
        return jnp.dot(rays_t[...], dense[p], preferred_element_type=F32)

    def backward(turn, norm):
        def halves(step):
            block = product(z_at(step))
            return block[:, :HV], block[:, HV:]

        def pack_both(unit, pair):
            pack(turn, unit, pair[0].T)
            pack(turn, unit + 1, pair[1].T)

        def keep(i, pair):
            relay[2 * i] = pair[0].T
            relay[2 * i + 1] = pair[1].T

        with jax.named_scope("products"):
            first = halves(4)
            second = halves(3)
            pack_both(4, first)
            if turn == 0:
                pl.semaphore_wait(barrier, 2 * (NZ - 1) + NQ - 1 + 1)
            send_units(turn, 4, 5)
            first = halves(-3)
            pack_both(0, second)
            send_units(turn, 0, 1)
            second = halves(1)
            pack_both(2, first)
            send_units(turn, 2, 3)
            if turn:
                meet_norm(turn - 1)
            else:
                give_norm(turn, norm)
            first = halves(-1)
            pack_both(6, second)
            send_units(turn, 6)
            second = halves(2)
            pack_both(8, first)
            send_units(turn, 8)
            first = halves(-2)
            keep(0, second)
            second = halves(0)
            keep(1, first)
            own_back[:HV] = second[0].T
            own_back[HV:] = second[1].T
        if turn:
            give_norm(turn, met_norm(turn - 1))
        with jax.named_scope("relay_wait"):
            await_units(turn, 0, 4)
        with jax.named_scope("relay"):
            pack(turn, 10, relay[0] + unpack(turn, 0) + unpack(turn, 4))
            send_units(turn, 10)
        with jax.named_scope("relay_wait"):
            await_units(turn, 3, 5)
        with jax.named_scope("relay"):
            pack(turn, 13, relay[3] + unpack(turn, 3) + unpack(turn, 5))
            send_units(turn, 13)
        with jax.named_scope("relay_wait"):
            await_units(turn, 1)
        with jax.named_scope("relay"):
            pack(turn, 11, relay[1] + unpack(turn, 1))
            send_units(turn, 11)
        with jax.named_scope("relay_wait"):
            await_units(turn, 2)
        with jax.named_scope("relay"):
            pack(turn, 12, relay[2] + unpack(turn, 2))
            send_units(turn, 12)
        if turn:
            forward_left(turn - 1)
        beta = take_norm(turn)
        with jax.named_scope("reduce_1"):
            await_units(turn, 6, 8)
            own_back[:HV] += unpack(turn, 6) + unpack(turn, 8)
            own_back[HV:] += unpack(turn, 7) + unpack(turn, 9)
        with jax.named_scope("reduce_2"):
            await_units(turn, 10, 13)
            await_units(turn, 11, 12)
        with jax.named_scope("reduce_3"):
            own_back[:HV] += unpack(turn, 10) + unpack(turn, 12)
            own_back[HV:] += unpack(turn, 11) + unpack(turn, 13)
        return beta

    def backward_left(turn):
        left(quant.at[turn], z_send)
        left(quant_scale.at[turn], zm_send)
        left(row_ss.at[turn, pl.ds(0, NZ - 1)], zs_send)
        if turn:
            left(rays.at[turn - 1, core, pl.ds(0, NQ - 1)], g_send)
            left(rays_ss.at[turn - 1, pl.ds(0, NQ - 1)], gs_send)
            left(rays.at[turn - 1, core], r_send)
            left(half_ss.at[turn - 1, 0], n_send)

    def forward_left(turn):
        left(high.at[turn, pl.ds(0, NZ - 1)], h_send)
        left(high_ss.at[turn, pl.ds(0, NZ - 1)], hs_send)
        left(part_out.at[turn], c_send)
        left(part_ss.at[turn, 0], k_send)
        left(fwd_out.at[turn, pl.ds(0, NQ - 1)], q_send)
        left(fwd_ss.at[turn, pl.ds(0, NQ - 1)], qs_send)

    def gather_copy(turn, k, receiving):
        step, block, part = GATHER[k]
        slot = z_at(block - step if receiving else block)
        rows_at = pl.ds(0, VB) if part is None else pl.ds(part * (VB // PIECES), VB // PIECES)
        view = high.at[turn, slot, rows_at]
        return remote(view, view, h_send, h_recv.at[k], z_id(step))

    def high_norm(turn, step, slot):
        return remote(high_ss.at[turn, z], high_ss.at[turn, slot], hs_send, hs_recv, z_id(step))

    def forward(turn, voxel):
        with jax.named_scope("gather"):
            top = jnp.maximum(jnp.max(jnp.abs(voxel), axis=0, keepdims=True), 1e-30)
            high[turn, z] = jnp.round(voxel * (32767.0 / top)).astype(jnp.int32).astype(jnp.int16)
            high_ss[turn, z, 0] = squares(voxel)
            high_ss[turn, z, 1] = top * (1.0 / 32767.0)
            for step in (4, 3, 5, 2, 6, 1, 7):
                high_norm(turn, step, z).start()
            for k in range(NEAR):
                gather_copy(turn, k, False).start()
            operand[z] = voxel.astype(BF16)
        for arrived, onward in enumerate(ONWARD):
            with jax.named_scope("gather_relay"):
                gather_copy(turn, arrived, True).wait_recv()
                for k in onward:
                    gather_copy(turn, k, False).start()
        with jax.named_scope("gather_1"):
            gather_copy(turn, NEAR - 2, True).wait_recv()
            gather_copy(turn, NEAR - 1, True).wait_recv()
            took(high_ss.at[turn, pl.ds(0, NZ - 1)], hs_recv)

        def widen(step):
            p = z_at(step)
            operand[p] = (high[turn, p].astype(jnp.int32).astype(F32) * high_ss[turn, p, 1]).astype(BF16)

        total = high_ss[turn, 0, 0]
        for i in range(1, NZ):
            total = total + high_ss[turn, i, 0]
        part_ss[turn, 0] = total
        core_norm = remote(part_ss.at[turn, 0], part_ss.at[turn, 1], k_send, k_recv, other)
        core_norm.start()

        with jax.named_scope("widen"):
            for step in (1, -1, 2, -2):
                widen(step)

        def product(at, steps):
            block = None
            for step in steps:
                p = z_at(step)
                term = jnp.dot(dense[p, at, :], operand[p], preferred_element_type=F32)
                block = term if block is None else block + term
            return block.reshape(-1, RB, Z)

        near = (0, 1, -1, 2, -2)
        far = (3, -3, 4)

        def theirs_at(i, count):
            return pl.ds(pl.multiple_of((1 - core) * HALF + i * count, 256), count)

        def ours_at(i, count):
            return pl.ds(pl.multiple_of(core * HALF + i * count, 256), count)

        def near_product(i, carry):
            at = pl.ds(i * CB, CB)
            part_out[turn, at] = product(theirs_at(i, 256), near)
            part_own[at] = product(ours_at(i, 256), near)
            return carry

        looped("near_product", 0, HALF // 256, near_product, 0)
        with jax.named_scope("give_alpha"):
            core_norm.wait_recv()
            chip_ss = part_ss[turn, 0] + part_ss[turn, 1]
            fwd_ss[turn, chip] = chip_ss
            fwd_ss[turn, NQ] = chip_ss
            for step in CHIPS:
                remote(fwd_ss.at[turn, NQ], fwd_ss.at[turn, chip], qs_send, qs_recv, chip_id(step)).start()

        with jax.named_scope("gather_3"):
            for k in range(NEAR, len(GATHER)):
                gather_copy(turn, k, True).wait_recv()
        with jax.named_scope("widen"):
            for step in (3, -3, 4):
                widen(step)


        def core_copy(i):
            at = pl.ds(i * FB, FB)
            return remote(part_out.at[turn, at], part_in.at[turn, at], c_send, c_recv, other)

        def theirs(i, carry):
            at = pl.ds(i * FB, FB)
            part_out[turn, at] += product(theirs_at(i, FAR), far)
            core_copy(i).start()
            return carry

        looped("theirs", 0, HALF // FAR, theirs, 0)
        def ours(i, carry):
            part_own[pl.ds(i * FB, FB)] += product(ours_at(i, FAR), far)
            return carry

        looped("ours", 0, HALF // FAR, ours, 0)
        with jax.named_scope("core_wait"):
            took(part_in.at[turn], c_recv)
        with jax.named_scope("give_rays"):
            for step in CHIPS:
                q = chip_peer(step)
                fwd_out[turn, q] = (part_own[q] + part_in[turn, q]).astype(BF16)
                remote(fwd_out.at[turn, q], fwd_in.at[turn, chip], q_send, q_recv, chip_id(step)).start()
        backward_left(turn)
        with jax.named_scope("take_rays"):
            took(fwd_ss.at[turn, pl.ds(0, NQ - 1)], qs_recv)
            took(fwd_in.at[turn, pl.ds(0, NQ - 1)], q_recv)
            rays_sum = part_own[chip] + part_in[turn, chip]
            for step in CHIPS:
                rays_sum = rays_sum + fwd_in[turn, chip_from(step)].astype(F32)
        alpha = jnp.sqrt(sum_rows(fwd_ss, turn, NQ) + EPSILON)
        return rays_sum, alpha

    def share_rays(turn, ray, with_data):
        if with_data:
            rays[turn, core, chip] = ray.astype(BF16)
        rays_ss[turn, chip] = squares(ray)

        with jax.named_scope("share"):
            if with_data:
                mine = rays.at[turn, core, chip]
                for step in CHIPS:
                    remote(mine, mine, g_send, g_recv, chip_id(step)).start()
            for step in CHIPS:
                remote(rays_ss.at[turn, chip], rays_ss.at[turn, chip], gs_send, gs_recv, chip_id(step)).start()
        if not with_data:
            with jax.named_scope("take_share"):
                took(rays_ss.at[turn, pl.ds(0, NQ - 1)], gs_recv)
            return sum_rows(rays_ss, turn, NQ)
        with jax.named_scope("take_share"):
            took(rays.at[turn, core, pl.ds(0, NQ - 1)], g_recv)
        data = remote(rays.at[turn, core], rays.at[turn, core], r_send, r_recv, other)
        back_data = remote(rays.at[turn, core], rays.at[turn, 1 - core], r_send, r_recv, other)
        data.start()

        def turned(c):
            for i in range(HALF // 256):
                part = rays[turn, c, i * CB : (i + 1) * CB].reshape(256, Z)
                first = pl.multiple_of(c * HALF + i * 256, 256)
                rays_t[:, pl.ds(first, 256)] = part.astype(F32).T.astype(BF16)

        turned(core)
        with jax.named_scope("core_rays"):
            back_data.wait_recv()
        turned(1 - core)
        return None

    def core_norm_copy(turn):
        return remote(half_ss.at[turn, 0], half_ss.at[turn, 1], n_send, n_recv, other)

    def meet_norm(turn):
        took(rays_ss.at[turn, pl.ds(0, NQ - 1)], gs_recv)
        half_ss[turn, 0] = sum_rows(rays_ss, turn, NQ)
        core_norm_copy(turn).start()

    def met_norm(turn):
        with jax.named_scope("met_norm"):
            core_norm_copy(turn).wait_recv()
        return half_ss[turn, 0] + half_ss[turn, 1]

    beta = backward(0, jnp.sum(first_ss, axis=0, keepdims=True))
    voxel = own_back[...] / beta
    share = sino[core * (HALF // 256) + chip // CB, pl.ds(pl.multiple_of(lax.rem(chip, CB) * RB, RB), RB), :]
    ray_vec = share / beta
    phi_bar = beta
    rho_bar = None
    scale = []
    steps = []
    turns = []
    for turn in range(ITERS):
        rays_sum, alpha = forward(turn, voxel)
        scale.append(alpha)
        if turn == 0:
            rho_bar = alpha
        else:
            theta = sine * alpha
            turns.append(theta / rho)
            rho_bar = -cosine * alpha
        ray_raw = rays_sum / alpha - alpha * ray_vec
        norm = share_rays(turn, ray_raw, turn + 1 < ITERS)
        if turn + 1 < ITERS:
            beta = backward(turn + 1, norm)
            rho = jnp.sqrt(rho_bar * rho_bar + beta * beta)
            cosine = rho_bar / rho
            sine = beta / rho
            phi = cosine * phi_bar
            phi_bar = sine * phi_bar
            steps.append(phi / rho)
            ray_vec = ray_raw / beta
            voxel = own_back[...] / beta - beta * (voxel / alpha)

    weight = [[None] * ITERS for _ in range(ITERS)]
    for k in range(ITERS):
        weight[k][k] = 1.0 / scale[k]
        for j in range(k):
            weight[k][j] = -turns[k - 1] * weight[k - 1][j]
    known = [steps[0] * weight[0][0] + steps[1] * weight[1][0], steps[1] * weight[1][1]]
    final = weight[ITERS - 1]

    place = z * 2 + core
    last_ss[0, place] = norm

    def last_copy(device):
        return remote(last_ss.at[0, place], last_ss.at[0, place], e_send, e_recv, device)

    def give_last(step, carry):
        last_copy(z_id(step)).start()
        last_copy(across_id(step)).start()
        return carry

    looped("give_last", 1, NZ, give_last, 0)
    last_copy(other).start()

    def combine(p, carry):
        at = pl.ds(pl.multiple_of(p * VB, VB), VB)
        base = step = None
        for k in range(ITERS):
            value = high[k, p].astype(jnp.int32).astype(F32) * high_ss[k, p, 1]
            step = final[k] * value if step is None else step + final[k] * value
            if k < len(known):
                base = known[k] * value if base is None else base + known[k] * value
        done[at, :] = base
        last[at, :] = step
        return carry

    looped("combine", 0, NZ, combine, 0)
    with jax.named_scope("take_last"):
        took(last_ss.at[0, pl.ds(0, 2 * NZ - 1)], e_recv)
    beta = jnp.sqrt(sum_rows(last_ss, 0, 2 * NZ) + EPSILON)
    rho = jnp.sqrt(rho_bar * rho_bar + beta * beta)
    cosine = rho_bar / rho
    sine = beta / rho
    rows[0:1, :] = (cosine * phi_bar) / rho
    rows[1:2, :] = sine * phi_bar

    forward_left(ITERS - 1)
    left(rays_ss.at[ITERS - 1, pl.ds(0, NQ - 1)], gs_send)
    left(last_ss.at[0, pl.ds(0, 2 * NZ - 1)], e_send)


def finish(done, last, rows, out, residual):
    out[...] = done[...] + rows[0:1, :] * last[...]
    residual[...] = rows[1:2, :]


def stay(array):
    return pltpu.with_memory_space_constraint(array, pltpu.HBM)


def body(tile_values, tile_rows, tile_cols, tile_count, sinogram):
    values = tile_values[0, 0]
    dma = pltpu.SemaphoreType.DMA
    vmem = pltpu.VMEM
    tiles = values.shape
    scratch = [
        vmem((tiles[0] + 1, *tiles[1:]), BF16),
        vmem((BLK // 256, 256, Z), F32),
        vmem((NZ, BLK, VB), BF16),
        vmem((Z, BLK), BF16),
        vmem((ITERS, UNITS, HV, Z), jnp.int16),
        vmem((ITERS, UNITS, 1, Z), F32),
        vmem((ITERS, UNITS, HV, Z), jnp.int16),
        vmem((ITERS, UNITS, 1, Z), F32),
        vmem((ITERS, NZ, 1, Z), F32),
        vmem((4, HV, Z), F32),
        vmem((VB, Z), F32),
        vmem((ITERS, NZ, VB, Z), jnp.int16),
        vmem((NZ, VB, Z), BF16),
        vmem((ITERS, NZ, 2, 1, Z), F32),
        vmem((NQ, RB, Z), F32),
        vmem((ITERS, NQ, RB, Z), F32),
        vmem((ITERS, NQ, RB, Z), F32),
        vmem((ITERS, 2, 1, Z), F32),
        vmem((ITERS, NQ, RB, Z), BF16),
        vmem((ITERS, NQ, RB, Z), BF16),
        vmem((ITERS, NQ + 1, 1, Z), F32),
        vmem((ITERS - 1, 2, NQ, RB, Z), BF16),
        vmem((ITERS, NQ, 1, Z), F32),
        vmem((ITERS, 2, 1, Z), F32),
        vmem((1, 2 * NZ, 1, Z), F32),
        vmem((2, 1, TILE), jnp.int32),
        vmem((8, TILE), jnp.int32),
        pltpu.SMEM((2, TILE), jnp.int32),
        dma((5,)),
    ]
    for send, recv in (
        ((), (UNITS,)),
        ((), (UNITS,)),
        ((), ()),
        ((), (len(GATHER),)),
        ((), ()),
        ((), ()),
        ((), ()),
        ((), ()),
        ((), ()),
        ((), ()),
        ((), ()),
        ((), ()),
        ((), ()),
        ((), ()),
    ):
        scratch += [dma(send), dma(recv)]
    in_vmem = pl.BlockSpec(memory_space=pltpu.VMEM)
    block = jax.ShapeDtypeStruct((BLK, Z), F32)
    done, last, rows = pl.pallas_call(
        kernel,
        out_shape=(block, block, jax.ShapeDtypeStruct((8, Z), F32)),
        in_specs=[
            pl.BlockSpec(memory_space=pltpu.SMEM),
            pl.BlockSpec(memory_space=pltpu.HBM),
            pl.BlockSpec(memory_space=pltpu.HBM),
            pl.BlockSpec(memory_space=pltpu.HBM),
            pl.BlockSpec(memory_space=pltpu.HBM),
        ],
        out_specs=(in_vmem, in_vmem, in_vmem),
        scratch_shapes=scratch,
        compiler_params=pltpu.CompilerParams(collective_id=0, has_side_effects=True, vmem_limit_bytes=48 * 1024 * 1024),
    )(tile_count, stay(tile_rows[0]), stay(tile_cols[0]), values, stay(sinogram.reshape(BLK // 256, 256, Z)))
    found, residual = pl.pallas_call(
        finish,
        out_shape=(block, jax.ShapeDtypeStruct((1, Z), F32)),
        in_specs=[in_vmem, in_vmem, in_vmem],
        out_specs=(in_vmem, in_vmem),
        compiler_params=pltpu.CompilerParams(vmem_limit_bytes=8 * 1024 * 1024),
    )(done, last, rows)
    return found, residual[0]


def solution(mesh):
    split = Mesh(mesh.devices.reshape(NZ, NX, NY, 2), ("row", "cx", "cy", "cc"))
    col = ("cx", "cy", "cc")
    placed = (
        P("row", col, None, None, None),
        P("row", col, None),
        P("row", col, None),
        P("row", col),
        P("row", None),
    )
    return jax.shard_map(body, mesh=split, in_specs=placed, out_specs=(P(col, None), P()), check_vma=False)
```
